256 devices in a mesh: gx: 32 (over y, z), gy: 8 (over x, core).
Axes of the slice: x: 4, y: 4, z: 8, core: 2. Of those that a mesh axis runs over, the one named last changes fastest.
Arguments:
- right_side: float32 [64, 128, 4, 3, 128], P('gx', 'gy'), may hold values from -6 to 6
- stencil: float32 [27, 3, 3], replicated, as said below
- class_scale: float32 [8], replicated, may hold values from 0.5 to 4
- material: int32 [64, 128, 128], P('gx', 'gy'), may hold values from 0 to 7
- boundary: int32 [64, 128, 128], P('gx', 'gy'), may hold values 0 or 1
- sign_bits: int32 [64, 128, 3, 128], P('gx', 'gy'), may hold values from 0 to 1
- sample_rows: int32 [32, 8, 128], P('gx', 'gy'), may hold values from 0 to 12287
Outputs:
- solution: float32 [64, 128, 4, 3, 128], P('gx', 'gy')
- residual: float32 [64, 128, 4, 3, 128], P('gx', 'gy')
The draws below stay inside these ranges and needn't reach their ends.
Inputs may be any that keep to these rules, and one draw needn't show every extreme that they name: In every row of the centre block stencil[13], the diagonal entry exceeds the sum of the magnitudes of all other entries of that row over all 27 blocks.
All inputs are finite; a program needn't handle non-finite values. No bound on the sum of `boundary` on one device may be relied on, other than what follows from the above.
Results may differ from the reference program's by a relative error of at most 0.0028.
Values sent between devices are 32-bit elements; how exact they have to be, the bound alone decides.
A program may use at most 64 MiB of HBM per device.

```python
import math
import jax
import jax.numpy as jnp
from jax import lax

CX = 2
CY = 16
NZ = 128
BW = 4
STEPS = 8
SK = 128
NCLASS = 8
NX = 64
NY = 128
N_GX = 32
N_GY = 8


def draw_stencil(key, part):
    subkeys = jax.random.split(jax.random.fold_in(key, 11), 4)
    rough = 0.4 * jax.random.normal(subkeys[0], (27, 3, 3), jnp.float32)
    pulled = jax.random.uniform(subkeys[1], (27, 1, 1), jnp.float32, 0.3, 1.0)
    identity = jnp.eye(3, dtype=jnp.float32)
    blocks = rough - 0.5 * pulled * identity
    centre_rough = 0.3 * jax.random.normal(subkeys[2], (3, 3), jnp.float32) * (1.0 - identity)
    others = jnp.sum(jnp.abs(blocks), axis=(0, 2)) - jnp.sum(jnp.abs(blocks[13]), axis=1) + jnp.sum(jnp.abs(centre_rough), axis=1)
    margin = jax.random.uniform(subkeys[3], (3,), jnp.float32, 0.5, 2.0)
    centre = centre_rough + jnp.diag(others + margin)
    blocks = blocks.at[13].set(centre)
    return blocks / jnp.mean(others + margin)


def place_ends(entries, key, low, largest):
    longest = entries.shape.index(max(entries.shape))
    spots = []
    for shift in (0, 1):
        where = [jax.random.randint(jax.random.fold_in(key, axis), (), 0, length) for axis, length in enumerate(entries.shape)]
        where[longest] = (where[longest] + shift) % entries.shape[longest]
        spots.append(tuple(where))
    return entries.at[spots[0]].set(low).at[spots[1]].set(largest)


def steps_of(key, dims, pieces, smallest, top_value):
    factor_of = 1.0
    for dim, blocks in pieces:
        steps = jax.random.uniform(jax.random.fold_in(jax.random.fold_in(key, 6), dim), (blocks,), jnp.float32, smallest / len(pieces), top_value / len(pieces))
        factor_of = factor_of * jnp.repeat(jnp.exp(steps), dims[dim] // blocks).reshape((-1,) + (1,) * (len(dims) - 1 - dim))
    return factor_of


def bell_draw(own_key, extent, width, limit, shards=(), held_as=jnp.bfloat16):
    factor_of = steps_of(own_key, extent, shards, -0.22, 0.18) if shards else 1.0
    drawn = jax.random.normal(own_key, extent, jnp.float32) * width * factor_of
    return jnp.minimum(jnp.maximum(drawn, -limit), limit).astype(held_as)


def setup_inputs(seed: int = 0) -> dict:
    arg_keys = jax.random.split(jax.random.key(seed), 8)
    return {
        "right_side": bell_draw(arg_keys[0], (NX, NY, BW, 3, NZ), 1.0, 6.0, ((0, 32), (1, 8)), jnp.float32),
        "stencil": draw_stencil(jax.random.fold_in(arg_keys[7], 71), 0),
        "class_scale": jnp.clip(jnp.exp(jax.random.uniform(arg_keys[2], (NCLASS,), jnp.float32, math.log(0.5), math.log(4.0))), 0.5, 4.0),
        "material": place_ends(jax.random.randint(arg_keys[3], (NX, NY, NZ), 0, NCLASS), jax.random.fold_in(arg_keys[3], 1), 0, NCLASS - 1).astype(jnp.int32),
        "boundary": place_ends((jax.random.randint(arg_keys[4], (NX, NY, NZ), 0, 16) < 1).astype(jnp.int32), jax.random.fold_in(arg_keys[4], 1), 0, 1),
        "sign_bits": place_ends(jax.random.randint(arg_keys[5], (NX, NY, 3, NZ), 0, 2), jax.random.fold_in(arg_keys[5], 1), 0, 1).astype(jnp.int32),
        "sample_rows": place_ends(jax.random.randint(arg_keys[6], (N_GX, N_GY, SK), 0, 3 * CX * CY * NZ), jax.random.fold_in(arg_keys[6], 1), 0, (3 * CX * CY * NZ) - 1).astype(jnp.int32),
    }


exact_mode = lax.Precision.HIGHEST

def hadamard_table():
    lanes = jnp.arange(128, dtype=jnp.int32)
    common = lanes[:, None] & lanes[None, :]
    parity = jnp.zeros((128, 128), jnp.int32)
    for bit in range(7):
        parity = parity + (common >> bit & 1)
    return (1 - 2 * (parity % 2)).astype(jnp.float32) / math.sqrt(128.0)

def material_scale(material, class_scale):
    scale_field = jnp.zeros(material.shape, jnp.float32)
    for number in range(class_scale.shape[0]):
        scale_field = scale_field + jnp.where(material == number, class_scale[number], jnp.float32(0.0))
    return scale_field

def operate(field, stencil, scale_field, boundary):
    padded = jnp.pad(field, ((1, 1), (1, 1), (0, 0), (0, 0), (1, 1)))
    extent_x, extent_y, extent_z = (field.shape[0], field.shape[1], field.shape[4])
    summed = jnp.zeros(field.shape, jnp.float32)
    for offset_x in range(3):
        for offset_y in range(3):
            for offset_z in range(3):
                shifted = padded[offset_x:offset_x + extent_x, offset_y:offset_y + extent_y, :, :, offset_z:offset_z + extent_z]
                coupling = stencil[offset_x * 9 + offset_y * 3 + offset_z]
                summed = summed + lax.optimization_barrier(jnp.sum(coupling[:, :, None] * shifted[:, :, :, None, :, :], axis=4))
    return jnp.where(boundary[:, :, None, None, :] == 1, field, scale_field[:, :, None, None, :] * summed)

def sketch_of(field, sign_bits, sample_rows, table):
    sign_field = (2 * sign_bits - 1).astype(jnp.float32)
    signed = field * sign_field[:, :, None, :, :]
    tiled = signed.reshape(NX, NY, BW, 3, NZ // 128, 128)
    plane = CY * 3 * NZ
    pick_x = sample_rows // plane
    rest_y = sample_rows % plane
    pick_y = rest_y // (3 * NZ)
    rest_c = rest_y % (3 * NZ)
    pick_comp = rest_c // NZ
    pick_z = rest_c % NZ
    global_x = pick_x + (jnp.arange(N_GX, dtype=jnp.int32) * CX)[:, None, None]
    global_y = pick_y + (jnp.arange(N_GY, dtype=jnp.int32) * CY)[None, :, None]
    chosen = tiled[global_x, global_y, :, pick_comp, pick_z // 128]
    table_rows = table[pick_z % 128]
    local_terms = lax.optimization_barrier(jnp.sum(chosen * table_rows[:, :, :, None, :], axis=-1))
    return lax.optimization_barrier(jnp.sum(local_terms, axis=(0, 1)))

def back_substitute(triangle, projected):
    count = triangle.shape[0]

    def one_row(step, unknowns):
        row = count - 1 - step
        line = triangle[row]
        total = jnp.dot(line[None, :], unknowns, precision=exact_mode)[0]
        value = (projected[row] - total) / line[row]
        return unknowns.at[row].set(value)
    return lax.fori_loop(0, count, one_row, jnp.zeros(projected.shape, jnp.float32))

def solve_small(matrix, rhs):
    count = matrix.shape[1]
    columns = matrix.T

    def one_column(column, state_pair):
        orthonormal, triangle = state_pair
        vector = columns[column]
        first_pass = jnp.dot(orthonormal.T, vector, precision=exact_mode)
        vector = vector - jnp.dot(orthonormal, first_pass, precision=exact_mode)
        second_pass = jnp.dot(orthonormal.T, vector, precision=exact_mode)
        vector = vector - jnp.dot(orthonormal, second_pass, precision=exact_mode)
        length = jnp.sqrt(jnp.sum(vector * vector) + 1e-06)
        orthonormal = orthonormal.at[:, column].set(vector / length)
        triangle = triangle.at[:, column].set((first_pass + second_pass).at[column].set(length))
        return (orthonormal, triangle)
    start = (jnp.zeros(matrix.shape, jnp.float32), jnp.zeros((count, count), jnp.float32))
    orthonormal, triangle = lax.fori_loop(0, count, one_column, start)
    projected = jnp.dot(orthonormal.T, rhs, precision=exact_mode)
    return back_substitute(triangle, projected)

def reference(right_side, stencil, class_scale, material, boundary, sign_bits, sample_rows):
    table = hadamard_table()
    scale_field = material_scale(material, class_scale)
    sketch_rhs = sketch_of(right_side, sign_bits, sample_rows, table)
    lengths = jnp.sqrt(lax.optimization_barrier(jnp.sum(sketch_rhs * sketch_rhs, axis=0)) + 1e-06)
    basis_block = right_side / lengths[None, None, :, None, None]
    sketch_basis = sketch_rhs / lengths
    blocks = []
    sketched_images = []
    for block_step in range(STEPS):
        operated = operate(basis_block, stencil, scale_field, boundary)
        sketch_image = sketch_of(operated, sign_bits, sample_rows, table)
        blocks.append(basis_block)
        sketched_images.append(sketch_image)
        if block_step + 1 < STEPS:
            coupling = jnp.dot(sketch_basis.T, sketch_image, precision=exact_mode)
            remainder = operated - jnp.einsum('xyicz,ij->xyjcz', basis_block, coupling, precision=exact_mode)
            sketch_remainder = sketch_of(remainder, sign_bits, sample_rows, table)
            norms = jnp.sqrt(lax.optimization_barrier(jnp.sum(sketch_remainder * sketch_remainder, axis=0)) + 1e-06)
            basis_block = remainder / norms[None, None, :, None, None]
            sketch_basis = sketch_remainder / norms
    matrix = jnp.concatenate(sketched_images, axis=1)
    weights = solve_small(matrix, sketch_rhs)
    solution = jnp.zeros(right_side.shape, jnp.float32)
    for block_step in range(STEPS):
        part_weights = weights[block_step * BW:(block_step + 1) * BW]
        solution = solution + jnp.einsum('xyicz,ij->xyjcz', blocks[block_step], part_weights, precision=exact_mode)
    residual = right_side - operate(solution, stencil, scale_field, boundary)
    return (solution, residual)
```

```python
import numpy as np
import jax
import jax.numpy as jnp
from jax import lax
from jax.experimental import pallas as pl
from jax.experimental.pallas import tpu as pltpu
from jax.sharding import PartitionSpec as P

STEPS = 8
NV = STEPS + 1
BW = 4
NROW = NV * BW
HIGH = lax.Precision.HIGHEST
MESH = pl.DeviceIdType.MESH

ROW0 = 8


def phase_tables():
    points = [
        (x * np.pi / 3, y * np.pi / 2, z * np.pi / 4)
        for x in range(4)
        for y in range(4)
        for z in range(8)
    ]
    offsets = [(o // 9 - 1, (o // 3) % 3 - 1, o % 3 - 1) for o in range(27)]
    phase = np.zeros((32, 128))
    phase[:27] = np.array(offsets) @ np.array(points).T
    keep = (np.arange(32) < 27)[:, None]
    return (np.cos(phase) * keep).astype(np.float32), (np.sin(phase) * keep).astype(np.float32)


def neighbours(n_gx, n_gy):
    gx, gy = lax.axis_index("gx"), lax.axis_index("gy")
    out = []
    for dx in (-1, 0, 1):
        for dy in (-1, 0, 1):
            if dx == 0 and dy == 0:
                continue
            ok = jnp.bool_(True)
            if dx < 0:
                ok = jnp.logical_and(ok, gx > 0)
            if dx > 0:
                ok = jnp.logical_and(ok, gx < n_gx - 1)
            if dy < 0:
                ok = jnp.logical_and(ok, gy > 0)
            if dy > 0:
                ok = jnp.logical_and(ok, gy < n_gy - 1)
            out.append((dx, dy, ok, {"gx": gx + dx, "gy": gy + dy}))
    return out


def spectrum(cos_ref, sin_ref, coef_ref, scale_ref):
    contract = (((0,), (0,)), ((), ()))
    coef = coef_ref[...]
    re = lax.dot_general(coef, cos_ref[...], contract, precision=HIGH, preferred_element_type=jnp.float32)
    im = lax.dot_general(coef, sin_ref[...], contract, precision=HIGH, preferred_element_type=jnp.float32)

    def row(t, i, j):
        return t[3 * i + j : 3 * i + j + 1]

    low, high = None, None
    for i in range(3):
        off = jnp.zeros((1, 128), jnp.float32)
        for j in range(3):
            if j != i:
                a = 0.5 * (row(re, i, j) + row(re, j, i))
                b = 0.5 * (row(im, i, j) - row(im, j, i))
                off = off + jnp.sqrt(a * a + b * b)
        lo, hi = row(re, i, i) - off, row(re, i, i) + off
        low = lo if low is None else jnp.minimum(low, lo)
        high = hi if high is None else jnp.maximum(high, hi)
    low = jnp.min(low, axis=1, keepdims=True)
    high = jnp.max(high, axis=1, keepdims=True)
    scales = scale_ref[0:1, :]
    smin = jnp.min(scales, axis=1, keepdims=True)
    smax = jnp.max(scales, axis=1, keepdims=True)
    low = jnp.minimum(jnp.minimum(low * smin, low * smax), 1.0)
    high = jnp.maximum(high * smax, 1.0)
    span = high - low
    low, high = low + 0.04 * span, high - 0.2 * span
    centre = 0.5 * (low + high)
    half = jnp.maximum(0.5 * (high - low), 1e-3 * high)
    return centre, half


def basis_kernel(
    n_gx, n_gy,
    stencil_ref, rhs_ref, factor_ref, signs_ref, sample_ref, cos_ref, sin_ref, coef_ref, scale_ref,
    basis_ref, sketch_ref, shape_ref,
    v, alpha, beta, mask, signed, send_sem, recv_sem, out_sem,
):
    around = neighbours(n_gx, n_gy)
    barrier = pltpu.get_barrier_semaphore()
    count = jnp.int32(0)
    for dx, dy, ok, device in around:
        count = count + jnp.where(ok, 1, 0)

        @pl.when(ok)
        def _():
            pl.semaphore_signal(barrier, inc=1, device_id=device, device_id_type=MESH)

    gx, gy = lax.axis_index("gx"), lax.axis_index("gy")

    v[0, :, :, 1:3, ROW0 : ROW0 + 16, :] = rhs_ref[...]

    def clear(k, carry):
        @pl.when(gx == 0)
        def _():
            v[k, :, :, 0] = jnp.zeros((BW, 3, 32, 128), jnp.float32)

        @pl.when(gx == n_gx - 1)
        def _():
            v[k, :, :, 3] = jnp.zeros((BW, 3, 32, 128), jnp.float32)

        @pl.when(gy == 0)
        def _():
            v[k, :, :, :, ROW0 - 1 : ROW0, :] = jnp.zeros((BW, 3, 4, 1, 128), jnp.float32)

        @pl.when(gy == n_gy - 1)
        def _():
            v[k, :, :, :, ROW0 + 16 : ROW0 + 17, :] = jnp.zeros((BW, 3, 4, 1, 128), jnp.float32)

        return carry

    lax.fori_loop(0, STEPS, clear, 0)
    pl.semaphore_wait(barrier, count)

    def halo(k, part, n):
        dx, dy, ok, device = around[n]
        xs = {-1: (1, 1, 3), 0: (1, 2, 1), 1: (2, 1, 0)}[dx]
        ys = {-1: (ROW0, 1, ROW0 + 16), 0: (ROW0, 16, ROW0), 1: (ROW0 + 15, 1, ROW0 - 1)}[dy]
        cols = pl.ds(2 * part, 2)
        return pltpu.make_async_remote_copy(
            src_ref=v.at[k, cols, :, pl.ds(xs[0], xs[1]), pl.ds(ys[0], ys[1]), :],
            dst_ref=v.at[k, cols, :, pl.ds(xs[2], xs[1]), pl.ds(ys[2], ys[1]), :],
            send_sem=send_sem.at[k, part, n],
            recv_sem=recv_sem.at[k, part, n],
            device_id=device,
            device_id_type=MESH,
        )

    def start(k, part):
        for n in range(8):
            @pl.when(around[n][2])
            def _():
                halo(k, part, n).start()

    def opposite(n):
        return 7 - n

    def arrive(k, part):
        for n in range(8):
            @pl.when(around[n][2])
            def _():
                halo(k, part, opposite(n)).wait_recv()

    def sent(k, part):
        for n in range(8):
            @pl.when(around[n][2])
            def _():
                halo(k, part, n).wait_send()

    start(0, 0)
    start(0, 1)

    centre, half = spectrum(cos_ref, sin_ref, coef_ref, scale_ref)
    inverse = 1.0 / half
    shape_ref[0:1, :] = jnp.broadcast_to(centre * inverse, (1, 128))
    shape_ref[1:2, :] = jnp.broadcast_to(inverse, (1, 128))
    shape_ref[2:8, :] = jnp.zeros((6, 128), jnp.float32)
    factor = factor_ref[...]
    inv3 = inverse.reshape(1, 1, 1)
    cen3 = centre.reshape(1, 1, 1)
    alpha[...] = factor * (2.0 * inv3)
    beta[...] = jnp.where(factor == 0.0, 2.0 * (1.0 - cen3), -2.0 * cen3) * inv3

    sample = sample_ref[...]
    piece = sample >> 7
    lane = sample & 127
    px = jnp.where(piece >= 48, 1, 0)
    rest = piece - 48 * px
    py = (rest * 171) >> 9
    pc = rest - 3 * py
    mine = pc * 32 + px * 16 + py
    pieces = lax.broadcasted_iota(jnp.int32, (96, 128), 0)
    chosen = jnp.where(pieces == mine, 1.0, 0.0)
    mask[...] = chosen
    common = lax.broadcasted_iota(jnp.int32, (128, 128), 0) & lane
    common = common ^ (common >> 4)
    common = common ^ (common >> 2)
    common = common ^ (common >> 1)
    hadamard = (1 - 2 * (common & 1)).astype(jnp.float32)
    signs = (2 * signs_ref[...] - 1).astype(jnp.float32).reshape(96, 128)
    picked = lax.dot_general(
        signs, chosen, (((0,), (0,)), ((), ())), precision=HIGH, preferred_element_type=jnp.float32
    )
    signed[...] = hadamard * picked

    def sketch(k):
        rows = []
        for b in range(BW):
            block = v[k, b, :, 1:3, ROW0 : ROW0 + 16, :].reshape(96, 128)
            spread = jnp.dot(block, signed[...], precision=HIGH, preferred_element_type=jnp.float32)
            rows.append(jnp.sum(spread * mask[...], axis=0, keepdims=True))
        rows = jnp.concatenate(rows, axis=0) * np.float32(1.0 / np.sqrt(128.0))
        sketch_ref[k] = rows

    def keep(k):
        return pltpu.make_async_copy(
            v.at[k, :, :, pl.ds(1, 2), pl.ds(ROW0, 16), :], basis_ref.at[k], out_sem.at[k]
        )

    keep(0).start()
    sketch(0)

    z_lane = lax.broadcasted_iota(jnp.int32, (1, 1, 1, 128), 3)
    not_last = z_lane < 127
    not_first = z_lane > 0

    def step(k, carry):
        first = k == 0
        own = jnp.where(first, jnp.float32(0.5), jnp.float32(1.0))
        old = jnp.where(first, jnp.float32(0.0), jnp.float32(1.0))
        before = jnp.maximum(k - 1, 0)
        for part in range(2):
            arrive(k, part)
            cols = pl.ds(2 * part, 2)
            total = [None, None, None]
            for dz in (-1, 1, 0):
                acc = list(total) if dz == 0 else [None, None, None]
                for dx in (-1, 0, 1):
                    for dy in (-1, 0, 1):
                        offset = 9 * (dx + 1) + 3 * (dy + 1) + (dz + 1)
                        for j in range(3):
                            field = v[k, cols, j, pl.ds(1 + dx, 2), pl.ds(ROW0 + dy, 16), :]
                            for i in range(3):
                                term = stencil_ref[offset * 9 + 3 * i + j] * field
                                acc[i] = term if acc[i] is None else acc[i] + term
                for i in range(3):
                    if dz == -1:
                        moved = jnp.where(not_first, pltpu.roll(acc[i], 1, 3), 0.0)
                        total[i] = moved
                    elif dz == 1:
                        moved = jnp.where(not_last, pltpu.roll(acc[i], 127, 3), 0.0)
                        total[i] = total[i] + moved
                    else:
                        total[i] = acc[i]
            for i in range(3):
                mid = v[k, cols, i, 1:3, ROW0 : ROW0 + 16, :]
                last = v[before, cols, i, 1:3, ROW0 : ROW0 + 16, :]
                value = own * (alpha[...] * total[i] + beta[...] * mid) - old * last
                v[k + 1, cols, i, 1:3, ROW0 : ROW0 + 16, :] = value

            @pl.when(k + 1 < STEPS)
            def _():
                start(k + 1, part)

        keep(k + 1).start()
        sketch(k + 1)
        for part in range(2):
            sent(k, part)
        return carry

    lax.fori_loop(0, STEPS, step, 0)

    def finish(k, carry):
        keep(k).wait()
        return carry

    lax.fori_loop(0, NV, finish, 0)


def solve_kernel(table_ref, shape_ref, basis_ref, solution_ref, residual_ref, rows, weights, sem):
    table = table_ref[...]
    ratio = shape_ref[0:1, 0:1]
    inverse = shape_ref[1:2, :]

    def block(k):
        return table[BW * k : BW * (k + 1)]

    images = [ratio * block(0) + block(1)]
    for k in range(1, STEPS):
        images.append(ratio * block(k) + 0.5 * (block(k + 1) + block(k - 1)))
    q = jnp.concatenate(images + [block(0)], axis=0)
    r = lax.broadcasted_iota(jnp.int32, (NROW, 128), 0)
    l = lax.broadcasted_iota(jnp.int32, (NROW, 128), 1)
    low = r < BW
    last = r >= BW * STEPS
    one, none = jnp.float32(1.0), jnp.float32(0.0)
    e = jnp.where(l == r, ratio, none)
    e = e + jnp.where(l == r + BW, jnp.where(low, one, 0.5), none)
    e = e + jnp.where(jnp.logical_and(l == r - BW, jnp.logical_not(low)), 0.5, none)
    e = e + jnp.where(l == r + 64, one, none)
    e = jnp.where(last, jnp.where(l == r - BW * STEPS, one, none), e)
    size = jnp.sum(q * q, axis=1, keepdims=True)
    unit = jnp.where(last[:, 0:1], one, lax.rsqrt(size + 1e-30))
    q = q * unit
    e = e * unit
    row = r[:, 0:1]
    weight = []
    for j in range(BW * STEPS):
        pivot = q[j : j + 1]
        dots = jnp.sum(q * pivot, axis=1, keepdims=True)
        scale = 1.0 / (dots[j : j + 1] + 1e-10)
        weight.append(scale)
        part = jnp.where(row > j, dots * scale, none)
        q = q - part * pivot
        e = e - part * e[j : j + 1]
    weight = jnp.concatenate(weight, axis=0)
    qs = q[: BW * STEPS]
    es = e[: BW * STEPS] * weight
    last_rows = e[BW * STEPS :]
    for _ in range(2):
        left = jnp.dot(last_rows[:, :NROW], table, precision=HIGH, preferred_element_type=jnp.float32)
        along = lax.dot_general(
            left, qs, (((1,), (1,)), ((), ())), precision=HIGH, preferred_element_type=jnp.float32
        )
        last_rows = last_rows - jnp.dot(along, es, precision=HIGH, preferred_element_type=jnp.float32)
    rows[0:BW] = last_rows
    rows[BW : 2 * BW] = -inverse * last_rows
    copy = pltpu.make_async_copy(rows, weights, sem)
    copy.start()
    copy.wait()
    for x in range(2):
        for b in range(BW):
            sol = jnp.zeros((3, 16, 128), jnp.float32)
            res = jnp.zeros((3, 16, 128), jnp.float32)
            for k in range(NV):
                for a in range(BW):
                    field = basis_ref[k, a, :, x]
                    res = res + weights[b, BW * k + a] * field
                    if k < STEPS:
                        sol = sol + weights[BW + b, 64 + BW * k + a] * field
            solution_ref[b, :, x] = sol
            residual_ref[b, :, x] = res


def solution(mesh):
    n_gx, n_gy = mesh.shape["gx"], mesh.shape["gy"]
    cosine, sine = phase_tables()

    def shards(right_side, stencil, class_scale, material, boundary, sign_bits, sample_rows):
        rhs = jnp.transpose(right_side, (2, 3, 0, 1, 4))
        signs = jnp.transpose(sign_bits, (2, 0, 1, 3))
        field = jnp.zeros(material.shape, jnp.float32)
        for number in range(class_scale.shape[0]):
            field = jnp.where(material == number, class_scale[number], field)
        factor = jnp.where(boundary == 1, jnp.float32(0.0), field)
        coef = jnp.pad(stencil.reshape(27, 9), ((0, 5), (0, 7)))
        scales = jnp.broadcast_to(jnp.tile(class_scale, 16)[None, :], (8, 128))
        vmem = pl.BlockSpec(memory_space=pltpu.VMEM)
        smem = pl.BlockSpec(memory_space=pltpu.SMEM)
        basis, sketch, shape = pl.pallas_call(
            lambda *refs: basis_kernel(n_gx, n_gy, *refs),
            out_shape=(
                jax.ShapeDtypeStruct((NV, BW, 3, 2, 16, 128), jnp.float32),
                jax.ShapeDtypeStruct((NV, BW, 128), jnp.float32),
                jax.ShapeDtypeStruct((8, 128), jnp.float32),
            ),
            in_specs=[smem] + [vmem] * 8,
            out_specs=(pl.BlockSpec(memory_space=pl.ANY), vmem, vmem),
            scratch_shapes=[
                pltpu.VMEM((NV, BW, 3, 4, 32, 128), jnp.float32),
                pltpu.VMEM((2, 16, 128), jnp.float32),
                pltpu.VMEM((2, 16, 128), jnp.float32),
                pltpu.VMEM((96, 128), jnp.float32),
                pltpu.VMEM((128, 128), jnp.float32),
                pltpu.SemaphoreType.DMA((STEPS, 2, 8)),
                pltpu.SemaphoreType.DMA((STEPS, 2, 8)),
                pltpu.SemaphoreType.DMA((NV,)),
            ],
            compiler_params=pltpu.CompilerParams(collective_id=0, has_side_effects=True),
            name="basis",
        )(stencil.reshape(-1), rhs, factor, signs, sample_rows.reshape(1, 128), cosine, sine, coef, scales)
        table = lax.psum(sketch.reshape(NROW, 128), ("gx", "gy"))
        out = jax.ShapeDtypeStruct((BW, 3, 2, 16, 128), jnp.float32)
        answer, residual = pl.pallas_call(
            solve_kernel,
            out_shape=(out, out),
            in_specs=[vmem] * 3,
            out_specs=(vmem, vmem),
            scratch_shapes=[
                pltpu.VMEM((8, 128), jnp.float32),
                pltpu.SMEM((8, 128), jnp.float32),
                pltpu.SemaphoreType.DMA,
            ],
            name="solve",
        )(table, shape, basis)
        back = lambda t: jnp.transpose(t, (2, 3, 0, 1, 4))
        return back(answer), back(residual)

    return jax.shard_map(
        shards,
        mesh=mesh,
        in_specs=(
            P("gx", "gy", None, None, None),
            P(),
            P(),
            P("gx", "gy", None),
            P("gx", "gy", None),
            P("gx", "gy", None, None),
            P("gx", "gy", None),
        ),
        out_specs=(P("gx", "gy", None, None, None), P("gx", "gy", None, None, None)),
        check_vma=False,
    )
```

```python
import numpy as np
import jax
import jax.numpy as jnp
from jax import lax
from jax.experimental import pallas as pl
from jax.experimental.pallas import tpu as pltpu
from jax.sharding import PartitionSpec as P

STEPS = 8
NCLASS = 8
NV = STEPS + 1
BW = 4
NROW = NV * BW
HIGH = lax.Precision.HIGHEST
MESH = pl.DeviceIdType.MESH

ROW0 = 8


def phase_tables():
    points = [
        (x * np.pi / 3, y * np.pi / 2, z * np.pi / 4)
        for x in range(4)
        for y in range(4)
        for z in range(8)
    ]
    offsets = [(o // 9 - 1, (o // 3) % 3 - 1, o % 3 - 1) for o in range(27)]
    phase = np.zeros((128, 128))
    phase[:27] = np.array(offsets) @ np.array(points).T
    keep = (np.arange(128) < 27)[:, None]
    return (np.cos(phase) * keep).astype(np.float32), (np.sin(phase) * keep).astype(np.float32)


def neighbours(n_gx, n_gy):
    gx, gy = lax.axis_index("gx"), lax.axis_index("gy")
    out = []
    for dx in (-1, 0, 1):
        for dy in (-1, 0, 1):
            if dx == 0 and dy == 0:
                continue
            ok = jnp.bool_(True)
            if dx < 0:
                ok = jnp.logical_and(ok, gx > 0)
            if dx > 0:
                ok = jnp.logical_and(ok, gx < n_gx - 1)
            if dy < 0:
                ok = jnp.logical_and(ok, gy > 0)
            if dy > 0:
                ok = jnp.logical_and(ok, gy < n_gy - 1)
            out.append((dx, dy, ok, {"gx": gx + dx, "gy": gy + dy}))
    return out


def spectrum(cos_ref, sin_ref, coef_ref, scale_ref):
    coef = coef_ref[...]
    re = jnp.dot(coef, cos_ref[...], precision=HIGH, preferred_element_type=jnp.float32)
    im = jnp.dot(coef, sin_ref[...], precision=HIGH, preferred_element_type=jnp.float32)

    def row(t, i, j):
        return t[3 * i + j : 3 * i + j + 1]

    low, high = None, None
    for i in range(3):
        off = jnp.zeros((1, 128), jnp.float32)
        for j in range(3):
            if j != i:
                a = 0.5 * (row(re, i, j) + row(re, j, i))
                b = 0.5 * (row(im, i, j) - row(im, j, i))
                off = off + jnp.sqrt(a * a + b * b)
        lo, hi = row(re, i, i) - off, row(re, i, i) + off
        low = lo if low is None else jnp.minimum(low, lo)
        high = hi if high is None else jnp.maximum(high, hi)
    low = jnp.min(low, axis=1, keepdims=True)
    high = jnp.max(high, axis=1, keepdims=True)
    smin = smax = scale_ref[0]
    for n in range(1, NCLASS):
        smin = jnp.minimum(smin, scale_ref[n])
        smax = jnp.maximum(smax, scale_ref[n])
    low = jnp.minimum(jnp.minimum(low * smin, low * smax), 1.0)
    high = jnp.maximum(high * smax, 1.0)
    span = high - low
    low, high = low + 0.04 * span, high - 0.2 * span
    centre = 0.5 * (low + high)
    half = jnp.maximum(0.5 * (high - low), 1e-3 * high)
    return centre, half


def least_squares(table, ratio, half):
    lane = lax.broadcasted_iota(jnp.int32, (BW, 128), 1)
    row = lax.broadcasted_iota(jnp.int32, (BW, 128), 0)
    none = jnp.float32(0.0)
    rhs = table[0:BW]
    up = jnp.where(lane < BW, none, jnp.where(lane < 2 * BW, jnp.float32(1.0), jnp.float32(0.5)))
    down = jnp.where(lane < NROW, jnp.float32(0.5), none)
    unit = jnp.where(lane == row, jnp.float32(1.0), none)

    def inverse_norm(t):
        return lax.rsqrt(jnp.sum(t * t, axis=1, keepdims=True) + 1e-6)

    scale = inverse_norm(rhs)
    u, p = rhs * scale, unit * scale
    images, coefs = [], []
    for k in range(STEPS):
        d = half * (ratio * p + up * pltpu.roll(p, BW, 1) + down * pltpu.roll(p, 128 - BW, 1))
        image = jnp.dot(d, table, precision=HIGH, preferred_element_type=jnp.float32)
        images.append(image)
        coefs.append(d + pltpu.roll(p, 64, 1))
        if k + 1 < STEPS:
            rest, prest = image, d
            for i in range(BW):
                coupling = jnp.sum(image * u[i : i + 1], axis=1, keepdims=True)
                rest = rest - coupling * u[i : i + 1]
                prest = prest - coupling * p[i : i + 1]
            scale = inverse_norm(rest)
            u, p = rest * scale, prest * scale

    q = jnp.concatenate(images + [rhs], axis=0)
    e = jnp.concatenate(coefs + [unit], axis=0)
    rows = lax.broadcasted_iota(jnp.int32, (NROW, 1), 0)
    lanes = lax.broadcasted_iota(jnp.int32, (1, 128), 1)
    is_rhs = rows >= BW * STEPS
    weight = jnp.zeros((1, 128), jnp.float32)
    square = jnp.zeros((1, 128), jnp.float32)
    along = jnp.zeros((BW, 128), jnp.float32)
    for j in range(BW * STEPS):
        pivot = q[j : j + 1]
        dots = jnp.sum(q * pivot, axis=1, keepdims=True)
        w = 1.0 / (dots[j : j + 1] + 1e-6)
        s = dots[j : j + 1] * w
        here = lanes == j
        weight = weight + jnp.where(here, w, none)
        square = square + jnp.where(here, s, none)
        part = jnp.where(rows > j, dots * w * jnp.where(is_rhs, jnp.float32(1.0), 2.0 - s), none)
        along = along + jnp.where(here, part[BW * STEPS :], none)
        q = q - part * pivot
        e = e - part * e[j : j + 1]
    nq = BW * STEPS
    qs, es, last = q[:nq], e[:nq], e[nq:]
    weight, square, along = weight[:, :nq], square[:, :nq], along[:, :nq]
    first = lane < NROW
    for _ in range(2):
        left = jnp.dot(jnp.where(first, last, none), table, precision=HIGH, preferred_element_type=jnp.float32)
        dots = lax.dot_general(
            left, qs, (((1,), (1,)), ((), ())), precision=HIGH, preferred_element_type=jnp.float32
        )
        change = dots * weight - along * (1.0 - square)
        along = along + change
        last = last - jnp.dot(change, es, precision=HIGH, preferred_element_type=jnp.float32)
    return last


def cycle_kernel(
    n_gx, n_gy, n_y, n_z,
    scale_ref, rhs_ref, stencil_ref, material_ref, boundary_ref, signs_ref, sample_ref, cos_ref, sin_ref,
    solution_ref, residual_ref,
    v, alpha, beta, mask, signed, coef, coef_s, table, rows, weights, part_a, part_b, part_c,
    send_sem, recv_sem, load_sem, sum_send, sum_recv, local_sem,
):
    gx, gy = lax.axis_index("gx"), lax.axis_index("gy")
    around = neighbours(n_gx, n_gy)
    here_y, here_z = gx // n_z, gx % n_z

    groups = (
        (part_a, 0, gy, n_gy, lambda i: {"gx": gx, "gy": i}),
        (part_b, 1, here_y, n_y, lambda i: {"gx": i * n_z + here_z, "gy": gy}),
        (part_c, 2, here_z, n_z, lambda i: {"gx": here_y * n_z + i, "gy": gy}),
    )

    loads = []
    for b in range(BW):
        for c in range(3):
            copy = pltpu.make_async_copy(
                rhs_ref.at[:, :, c, b, :], v.at[0, b, c, pl.ds(1, 2), pl.ds(ROW0, 16), :], load_sem.at[3 * b + c]
            )
            copy.start()
            loads.append(copy)

    barrier = pltpu.get_barrier_semaphore()
    count = jnp.int32(0)
    for dx, dy, ok, device in around:
        count = count + jnp.where(ok, 1, 0)

        @pl.when(ok)
        def _():
            pl.semaphore_signal(barrier, inc=1, device_id=device, device_id_type=MESH)

    for _, _, me, size, device in groups:
        count = count + (size - 1)
        for d in range(1, size):
            pl.semaphore_signal(barrier, inc=1, device_id=device((me + d) % size), device_id_type=MESH)

    def clear(k, carry):
        @pl.when(gx == 0)
        def _():
            v[k, :, :, 0] = jnp.zeros((BW, 3, 32, 128), jnp.float32)

        @pl.when(gx == n_gx - 1)
        def _():
            v[k, :, :, 3] = jnp.zeros((BW, 3, 32, 128), jnp.float32)

        @pl.when(gy == 0)
        def _():
            v[k, :, :, :, ROW0 - 1 : ROW0, :] = jnp.zeros((BW, 3, 4, 1, 128), jnp.float32)

        @pl.when(gy == n_gy - 1)
        def _():
            v[k, :, :, :, ROW0 + 16 : ROW0 + 17, :] = jnp.zeros((BW, 3, 4, 1, 128), jnp.float32)

        return carry

    lax.fori_loop(0, STEPS, clear, 0)
    table[...] = jnp.zeros((128, 128), jnp.float32)
    for copy in loads:
        copy.wait()
    pl.semaphore_wait(barrier, count)

    def halo(k, b, n):
        dx, dy, ok, device = around[n]
        xs = {-1: (1, 1, 3), 0: (1, 2, 1), 1: (2, 1, 0)}[dx]
        ys = {-1: (ROW0, 1, ROW0 + 16), 0: (ROW0, 16, ROW0), 1: (ROW0 + 15, 1, ROW0 - 1)}[dy]
        return pltpu.make_async_remote_copy(
            src_ref=v.at[k, b, :, pl.ds(xs[0], xs[1]), pl.ds(ys[0], ys[1]), :],
            dst_ref=v.at[k, b, :, pl.ds(xs[2], xs[1]), pl.ds(ys[2], ys[1]), :],
            send_sem=send_sem.at[k, b, n],
            recv_sem=recv_sem.at[k, b, n],
            device_id=device,
            device_id_type=MESH,
        )

    def start(k, b):
        for n in range(8):
            @pl.when(around[n][2])
            def _():
                halo(k, b, n).start()

    def arrive(k, b):
        for n in range(8):
            @pl.when(around[n][2])
            def _():
                halo(k, b, 7 - n).wait_recv()

    def sent(k, b):
        for n in range(8):
            @pl.when(around[n][2])
            def _():
                halo(k, b, n).wait_send()

    def piece(group, k, source, d, target):
        buffer, stage, _, _, device = group
        return pltpu.make_async_remote_copy(
            src_ref=buffer.at[k, source],
            dst_ref=buffer.at[k, source],
            send_sem=sum_send.at[stage, k, d],
            recv_sem=sum_recv.at[stage, k, source],
            device_id=device(target),
            device_id_type=MESH,
        )

    def spread(group, k, value):
        buffer, _, me, size, _ = group
        buffer[k, me] = value
        for d in range(1, size):
            piece(group, k, me, d, (me + d) % size).start()

    def gather(group, k):
        buffer, _, me, size, _ = group
        for d in range(1, size):
            source = (me + d) % size
            piece(group, k, source, d, source).wait_recv()
        value = buffer[k, 0]
        for i in range(1, size):
            value = value + buffer[k, i]
        for d in range(1, size):
            piece(group, k, me, d, (me + d) % size).wait_send()
        return value

    def advance(stage, k):
        value = gather(groups[stage], k)
        if stage < 2:
            spread(groups[stage + 1], k, value)
        else:
            table[pl.ds(BW * k, BW), :] = value

    for b in range(BW):
        start(0, b)

    coef[...] = jnp.zeros((16, 128), jnp.float32)
    for i in range(3):
        for j in range(3):
            coef[3 * i + j : 3 * i + j + 1, 0:27] = stencil_ref[i, j : j + 1, :]
    copy = pltpu.make_async_copy(coef, coef_s, local_sem)
    copy.start()
    centre, half = spectrum(cos_ref, sin_ref, coef, scale_ref)
    inverse = 1.0 / half
    inv3 = inverse.reshape(1, 1, 1)
    cen3 = centre.reshape(1, 1, 1)
    material = material_ref[...]
    factor = jnp.zeros((2, 16, 128), jnp.float32)
    for n in range(NCLASS):
        factor = jnp.where(material == n, scale_ref[n], factor)
    fixed = boundary_ref[...] == 1
    alpha[...] = jnp.where(fixed, 0.0, factor * (2.0 * inv3))
    beta[...] = jnp.where(fixed, 2.0 * (1.0 - cen3), -2.0 * cen3) * inv3

    sample = sample_ref[...]
    spot = sample >> 7
    lane = sample & 127
    px = jnp.where(spot >= 48, 1, 0)
    rest = spot - 48 * px
    py = (rest * 171) >> 9
    pc = rest - 3 * py
    mine = pc * 32 + px * 16 + py
    spots = lax.broadcasted_iota(jnp.int32, (96, 128), 0)
    chosen = jnp.where(spots == mine, 1.0, 0.0)
    mask[...] = chosen * np.float32(1.0 / np.sqrt(128.0))
    common = lax.broadcasted_iota(jnp.int32, (128, 128), 0) & lane
    common = common ^ (common >> 4)
    common = common ^ (common >> 2)
    common = common ^ (common >> 1)
    hadamard = (1 - 2 * (common & 1)).astype(jnp.float32)
    signs = jnp.concatenate([signs_ref[x, c] for c in range(3) for x in range(2)], axis=0)
    signs = (2 * signs - 1).astype(jnp.float32)
    picked = lax.dot_general(
        signs, chosen, (((0,), (0,)), ((), ())), precision=HIGH, preferred_element_type=jnp.float32
    )
    signed[...] = hadamard * picked

    def sketch(k):
        out = []
        for b in range(BW):
            block = v[k, b, :, 1:3, ROW0 : ROW0 + 16, :].reshape(96, 128)
            spread_out = jnp.dot(block, signed[...], precision=HIGH, preferred_element_type=jnp.float32)
            out.append(jnp.sum(spread_out * mask[...], axis=0, keepdims=True))
        spread(groups[0], k, jnp.concatenate(out, axis=0))

    sketch(0)
    copy.wait()

    z_lane = lax.broadcasted_iota(jnp.int32, (1, 1, 128), 2)
    not_last = z_lane < 127
    not_first = z_lane > 0

    def step(k, carry):
        first = k == 0
        own = jnp.where(first, jnp.float32(0.5), jnp.float32(1.0))
        old = jnp.where(first, jnp.float32(0.0), jnp.float32(1.0))
        before = jnp.maximum(k - 1, 0)

        def column(b, carry):
            arrive(k, b)
            total = [None, None, None]
            for dz in (-1, 1, 0):
                acc = list(total) if dz == 0 else [None, None, None]
                for dx in (-1, 0, 1):
                    for dy in (-1, 0, 1):
                        offset = 9 * (dx + 1) + 3 * (dy + 1) + (dz + 1)
                        for j in range(3):
                            field = v[k, b, j, pl.ds(1 + dx, 2), pl.ds(ROW0 + dy, 16), :]
                            for i in range(3):
                                term = coef_s[3 * i + j, offset] * field
                                acc[i] = term if acc[i] is None else acc[i] + term
                for i in range(3):
                    if dz == -1:
                        total[i] = jnp.where(not_first, pltpu.roll(acc[i], 1, 2), 0.0)
                    elif dz == 1:
                        total[i] = total[i] + jnp.where(not_last, pltpu.roll(acc[i], 127, 2), 0.0)
                    else:
                        total[i] = acc[i]
            for i in range(3):
                mid = v[k, b, i, 1:3, ROW0 : ROW0 + 16, :]
                last = v[before, b, i, 1:3, ROW0 : ROW0 + 16, :]
                v[k + 1, b, i, 1:3, ROW0 : ROW0 + 16, :] = (
                    own * (alpha[...] * total[i] + beta[...] * mid) - old * last
                )

            @pl.when(k + 1 < STEPS)
            def _():
                start(k + 1, b)

            return carry

        lax.fori_loop(0, BW, column, 0)
        sketch(k + 1)
        advance(0, k)

        @pl.when(k >= 1)
        def _():
            advance(1, k - 1)

        @pl.when(k >= 2)
        def _():
            advance(2, k - 2)

        def drain(b, carry):
            sent(k, b)
            return carry

        lax.fori_loop(0, BW, drain, 0)
        return carry

    lax.fori_loop(0, STEPS, step, 0)
    advance(0, STEPS)
    advance(1, STEPS - 1)
    advance(2, STEPS - 2)
    advance(1, STEPS)
    advance(2, STEPS - 1)
    advance(2, STEPS)

    rows[0:BW] = least_squares(table[...], centre * inverse, half)
    copy = pltpu.make_async_copy(rows, weights, local_sem)
    copy.start()
    copy.wait()

    def combine(b, carry):
        for x in range(2):
            sol = jnp.zeros((3, 16, 128), jnp.float32)
            res = jnp.zeros((3, 16, 128), jnp.float32)
            for k in range(NV):
                for a in range(BW):
                    field = v[k, a, :, 1 + x, ROW0 : ROW0 + 16, :]
                    res = res + weights[b, BW * k + a] * field
                    if k < STEPS:
                        sol = sol - weights[b, 64 + BW * k + a] * field
            solution_ref[b, :, x] = sol
            residual_ref[b, :, x] = res
        return carry

    lax.fori_loop(0, BW, combine, 0)


def solution(mesh):
    n_gx, n_gy = mesh.shape["gx"], mesh.shape["gy"]
    n_z = 8 if n_gx % 8 == 0 else n_gx
    n_y = n_gx // n_z
    cosine, sine = phase_tables()

    def shards(right_side, stencil, class_scale, material, boundary, sign_bits, sample_rows):
        rhs = jnp.transpose(right_side, (0, 1, 3, 2, 4))
        signs = jnp.transpose(sign_bits, (0, 2, 1, 3))
        blocks = jnp.transpose(stencil, (1, 2, 0))
        vmem = pl.BlockSpec(memory_space=pltpu.VMEM)
        smem = pl.BlockSpec(memory_space=pltpu.SMEM)
        hbm = pl.BlockSpec(memory_space=pl.ANY)
        out = jax.ShapeDtypeStruct((BW, 3, 2, 16, 128), jnp.float32)
        most = max(n_gy, n_y, n_z)
        answer, residual = pl.pallas_call(
            lambda *refs: cycle_kernel(n_gx, n_gy, n_y, n_z, *refs),
            out_shape=(out, out),
            in_specs=[smem, hbm] + [vmem] * 7,
            out_specs=(vmem, vmem),
            scratch_shapes=[
                pltpu.VMEM((NV, BW, 3, 4, 32, 128), jnp.float32),
                pltpu.VMEM((2, 16, 128), jnp.float32),
                pltpu.VMEM((2, 16, 128), jnp.float32),
                pltpu.VMEM((96, 128), jnp.float32),
                pltpu.VMEM((128, 128), jnp.float32),
                pltpu.VMEM((16, 128), jnp.float32),
                pltpu.SMEM((16, 128), jnp.float32),
                pltpu.VMEM((128, 128), jnp.float32),
                pltpu.VMEM((8, 128), jnp.float32),
                pltpu.SMEM((8, 128), jnp.float32),
                pltpu.VMEM((NV, n_gy, BW, 128), jnp.float32),
                pltpu.VMEM((NV, n_y, BW, 128), jnp.float32),
                pltpu.VMEM((NV, n_z, BW, 128), jnp.float32),
                pltpu.SemaphoreType.DMA((STEPS, BW, 8)),
                pltpu.SemaphoreType.DMA((STEPS, BW, 8)),
                pltpu.SemaphoreType.DMA((3 * BW,)),
                pltpu.SemaphoreType.DMA((3, NV, most)),
                pltpu.SemaphoreType.DMA((3, NV, most)),
                pltpu.SemaphoreType.DMA,
            ],
            compiler_params=pltpu.CompilerParams(collective_id=0, has_side_effects=True),
            name="cycle",
        )(
            class_scale, rhs, blocks, material, boundary, signs, sample_rows.reshape(1, 128),
            cosine, sine,
        )
        back = lambda t: jnp.transpose(t, (2, 3, 0, 1, 4))
        return back(answer), back(residual)

    return jax.shard_map(
        shards,
        mesh=mesh,
        in_specs=(
            P("gx", "gy", None, None, None),
            P(),
            P(),
            P("gx", "gy", None),
            P("gx", "gy", None),
            P("gx", "gy", None, None),
            P("gx", "gy", None),
        ),
        out_specs=(P("gx", "gy", None, None, None), P("gx", "gy", None, None, None)),
        check_vma=False,
    )
```

```python
import numpy as np
import jax
import jax.numpy as jnp
from jax import lax
from jax.experimental import pallas as pl
from jax.experimental.pallas import tpu as pltpu
from jax.sharding import PartitionSpec as P

STEPS = 8
NCLASS = 8
NV = STEPS + 1
BW = 4
NROW = NV * BW
HIGH = lax.Precision.HIGHEST
MESH = pl.DeviceIdType.MESH

ROW0 = 8
OWN = slice(2, 4)
PAIRS = STEPS // 2
GROUPS = PAIRS + 1
FIXED = -1.0


def phase_tables():
    points = [
        (x * np.pi / 3, y * np.pi / 2, z * np.pi / 4)
        for x in range(4)
        for y in range(4)
        for z in range(8)
    ]
    offsets = [(o // 9 - 1, (o // 3) % 3 - 1, o % 3 - 1) for o in range(27)]
    phase = np.zeros((128, 128))
    phase[:27] = np.array(offsets) @ np.array(points).T
    keep = (np.arange(128) < 27)[:, None]
    return (np.cos(phase) * keep).astype(np.float32), (np.sin(phase) * keep).astype(np.float32)


def neighbours(n_gx, n_gy):
    gx, gy = lax.axis_index("gx"), lax.axis_index("gy")
    out = []
    for dx in (-1, 0, 1):
        for dy in (-1, 0, 1):
            if dx == 0 and dy == 0:
                continue
            ok = jnp.bool_(True)
            if dx < 0:
                ok = jnp.logical_and(ok, gx > 0)
            if dx > 0:
                ok = jnp.logical_and(ok, gx < n_gx - 1)
            if dy < 0:
                ok = jnp.logical_and(ok, gy > 0)
            if dy > 0:
                ok = jnp.logical_and(ok, gy < n_gy - 1)
            out.append((dx, dy, ok, {"gx": gx + dx, "gy": gy + dy}))
    return out


def spectrum(cos_ref, sin_ref, coef_ref, scale_ref):
    coef = coef_ref[...]
    re = jnp.dot(coef, cos_ref[...], precision=HIGH, preferred_element_type=jnp.float32)
    im = jnp.dot(coef, sin_ref[...], precision=HIGH, preferred_element_type=jnp.float32)

    def row(t, i, j):
        return t[3 * i + j : 3 * i + j + 1]

    low, high = None, None
    for i in range(3):
        off = jnp.zeros((1, 128), jnp.float32)
        for j in range(3):
            if j != i:
                a = 0.5 * (row(re, i, j) + row(re, j, i))
                b = 0.5 * (row(im, i, j) - row(im, j, i))
                off = off + jnp.sqrt(a * a + b * b)
        lo, hi = row(re, i, i) - off, row(re, i, i) + off
        low = lo if low is None else jnp.minimum(low, lo)
        high = hi if high is None else jnp.maximum(high, hi)
    low = jnp.min(low, axis=1, keepdims=True)
    high = jnp.max(high, axis=1, keepdims=True)
    smin = smax = scale_ref[0]
    for n in range(1, NCLASS):
        smin = jnp.minimum(smin, scale_ref[n])
        smax = jnp.maximum(smax, scale_ref[n])
    low = jnp.minimum(jnp.minimum(low * smin, low * smax), 1.0)
    high = jnp.maximum(high * smax, 1.0)
    span = high - low
    low, high = low + 0.04 * span, high - 0.2 * span
    centre = 0.5 * (low + high)
    half = jnp.maximum(0.5 * (high - low), 1e-3 * high)
    return centre, half


def least_squares(table, ratio, half):
    lane = lax.broadcasted_iota(jnp.int32, (BW, 128), 1)
    row = lax.broadcasted_iota(jnp.int32, (BW, 128), 0)
    none = jnp.float32(0.0)
    rhs = table[BW : 2 * BW]
    up = jnp.where(lane < 2 * BW, none, jnp.where(lane < 3 * BW, jnp.float32(1.0), jnp.float32(0.5)))
    down = jnp.where(jnp.logical_and(lane >= BW, lane < NROW + BW), jnp.float32(0.5), none)
    unit = jnp.where(lane == row + BW, jnp.float32(1.0), none)

    def inverse_norm(t):
        return lax.rsqrt(jnp.sum(t * t, axis=1, keepdims=True) + 1e-6)

    scale = inverse_norm(rhs)
    u, p = rhs * scale, unit * scale
    images, coefs = [], []
    for k in range(STEPS):
        d = half * (ratio * p + up * pltpu.roll(p, BW, 1) + down * pltpu.roll(p, 128 - BW, 1))
        image = jnp.dot(d, table, precision=HIGH, preferred_element_type=jnp.float32)
        images.append(image)
        coefs.append(d + pltpu.roll(p, 64, 1))
        if k + 1 < STEPS:
            rest, prest = image, d
            for i in range(BW):
                coupling = jnp.sum(image * u[i : i + 1], axis=1, keepdims=True)
                rest = rest - coupling * u[i : i + 1]
                prest = prest - coupling * p[i : i + 1]
            scale = inverse_norm(rest)
            u, p = rest * scale, prest * scale

    q = jnp.concatenate(images + [rhs], axis=0)
    e = jnp.concatenate(coefs + [unit], axis=0)
    rows = lax.broadcasted_iota(jnp.int32, (NROW, 1), 0)
    lanes = lax.broadcasted_iota(jnp.int32, (1, 128), 1)
    is_rhs = rows >= BW * STEPS
    weight = jnp.zeros((1, 128), jnp.float32)
    square = jnp.zeros((1, 128), jnp.float32)
    along = jnp.zeros((BW, 128), jnp.float32)
    for j in range(BW * STEPS):
        pivot = q[j : j + 1]
        dots = jnp.sum(q * pivot, axis=1, keepdims=True)
        w = 1.0 / (dots[j : j + 1] + 1e-6)
        s = dots[j : j + 1] * w
        here = lanes == j
        weight = weight + jnp.where(here, w, none)
        square = square + jnp.where(here, s, none)
        part = jnp.where(rows > j, dots * w * jnp.where(is_rhs, jnp.float32(1.0), 2.0 - s), none)
        along = along + jnp.where(here, part[BW * STEPS :], none)
        q = q - part * pivot
        e = e - part * e[j : j + 1]
    nq = BW * STEPS
    qs, es, last = q[:nq], e[:nq], e[nq:]
    weight, square, along = weight[:, :nq], square[:, :nq], along[:, :nq]
    first = lane < NROW + BW
    for _ in range(1):
        left = jnp.dot(jnp.where(first, last, none), table, precision=HIGH, preferred_element_type=jnp.float32)
        dots = lax.dot_general(
            left, qs, (((1,), (1,)), ((), ())), precision=HIGH, preferred_element_type=jnp.float32
        )
        change = dots * weight - along * (1.0 - square)
        along = along + change
        last = last - jnp.dot(change, es, precision=HIGH, preferred_element_type=jnp.float32)
    return last


def cycle_kernel(
    n_gx, n_gy, n_y, n_z,
    scale_ref, rhs_ref, stencil_ref, material_ref, boundary_ref, signs_ref, sample_ref, cos_ref, sin_ref,
    solution_ref, residual_ref,
    v, factor, alpha, beta, mask, signed, coef, coef_s, table, rows, weights, part_a, part_b, part_c,
    send_sem, recv_sem, factor_send, factor_recv, load_sem, sum_send, sum_recv, local_sem,
):
    gx, gy = lax.axis_index("gx"), lax.axis_index("gy")
    around = neighbours(n_gx, n_gy)
    here_y, here_z = gx // n_z, gx % n_z

    groups = (
        (part_a, 0, gy, n_gy, lambda i: {"gx": gx, "gy": i}),
        (part_b, 1, here_y, n_y, lambda i: {"gx": i * n_z + here_z, "gy": gy}),
        (part_c, 2, here_z, n_z, lambda i: {"gx": here_y * n_z + i, "gy": gy}),
    )

    loads = []
    for b in range(BW):
        for c in range(3):
            copy = pltpu.make_async_copy(
                rhs_ref.at[:, :, c, b, :], v.at[0, b, c, pl.ds(2, 2), pl.ds(ROW0, 16), :], load_sem.at[3 * b + c]
            )
            copy.start()
            loads.append(copy)

    barrier = pltpu.get_barrier_semaphore()
    count = jnp.int32(0)
    for dx, dy, ok, device in around:
        count = count + jnp.where(ok, 1, 0)

        @pl.when(ok)
        def _():
            pl.semaphore_signal(barrier, inc=1, device_id=device, device_id_type=MESH)

    for _, _, me, size, device in groups:
        count = count + (size - 1)
        for d in range(1, size):
            pl.semaphore_signal(barrier, inc=1, device_id=device((me + d) % size), device_id_type=MESH)

    def clear(t, carry):
        k = 2 * t

        @pl.when(gx == 0)
        def _():
            v[k, :, :, 0:2] = jnp.zeros((BW, 3, 2, 32, 128), jnp.float32)

        @pl.when(gx == n_gx - 1)
        def _():
            v[k, :, :, 4:6] = jnp.zeros((BW, 3, 2, 32, 128), jnp.float32)

        @pl.when(gy == 0)
        def _():
            v[k, :, :, :, ROW0 - 2 : ROW0, :] = jnp.zeros((BW, 3, 6, 2, 128), jnp.float32)

        @pl.when(gy == n_gy - 1)
        def _():
            v[k, :, :, :, ROW0 + 16 : ROW0 + 18, :] = jnp.zeros((BW, 3, 6, 2, 128), jnp.float32)

        return carry

    lax.fori_loop(0, PAIRS, clear, 0)

    @pl.when(gx == 0)
    def _():
        factor[0] = jnp.zeros((32, 128), jnp.float32)

    @pl.when(gx == n_gx - 1)
    def _():
        factor[3] = jnp.zeros((32, 128), jnp.float32)

    @pl.when(gy == 0)
    def _():
        factor[:, ROW0 - 1 : ROW0, :] = jnp.zeros((4, 1, 128), jnp.float32)

    @pl.when(gy == n_gy - 1)
    def _():
        factor[:, ROW0 + 16 : ROW0 + 17, :] = jnp.zeros((4, 1, 128), jnp.float32)

    material = material_ref[...]
    scales = jnp.zeros((2, 16, 128), jnp.float32)
    for n in range(NCLASS):
        scales = jnp.where(material == n, scale_ref[n], scales)
    factor[1:3, ROW0 : ROW0 + 16, :] = jnp.where(boundary_ref[...] == 1, FIXED, scales)
    table[...] = jnp.zeros((128, 128), jnp.float32)
    for copy in loads:
        copy.wait()
    pl.semaphore_wait(barrier, count)

    def halo(k, b, n):
        dx, dy, ok, device = around[n]
        plane = {-1: 4, 0: 2, 1: 0}[dx]
        ys = {-1: (ROW0, 2, ROW0 + 16), 0: (ROW0, 16, ROW0), 1: (ROW0 + 14, 2, ROW0 - 2)}[dy]
        return pltpu.make_async_remote_copy(
            src_ref=v.at[k, b, :, pl.ds(2, 2), pl.ds(ys[0], ys[1]), :],
            dst_ref=v.at[k, b, :, pl.ds(plane, 2), pl.ds(ys[2], ys[1]), :],
            send_sem=send_sem.at[k // 2, b, n],
            recv_sem=recv_sem.at[k // 2, b, n],
            device_id=device,
            device_id_type=MESH,
        )

    def edge(n):
        dx, dy, ok, device = around[n]
        xs = {-1: (1, 1, 3), 0: (1, 2, 1), 1: (2, 1, 0)}[dx]
        ys = {-1: (ROW0, 1, ROW0 + 16), 0: (ROW0, 16, ROW0), 1: (ROW0 + 15, 1, ROW0 - 1)}[dy]
        return pltpu.make_async_remote_copy(
            src_ref=factor.at[pl.ds(xs[0], xs[1]), pl.ds(ys[0], ys[1]), :],
            dst_ref=factor.at[pl.ds(xs[2], xs[1]), pl.ds(ys[2], ys[1]), :],
            send_sem=factor_send.at[n],
            recv_sem=factor_recv.at[n],
            device_id=device,
            device_id_type=MESH,
        )

    def start(k, b):
        for n in range(8):
            @pl.when(around[n][2])
            def _():
                halo(k, b, n).start()

    def arrive(k, b):
        for n in range(8):
            @pl.when(around[n][2])
            def _():
                halo(k, b, 7 - n).wait_recv()

    def sent(k, b):
        for n in range(8):
            @pl.when(around[n][2])
            def _():
                halo(k, b, n).wait_send()

    def piece(group, k, source, d, target):
        buffer, stage, _, _, device = group
        return pltpu.make_async_remote_copy(
            src_ref=buffer.at[k, source],
            dst_ref=buffer.at[k, source],
            send_sem=sum_send.at[stage, k, d],
            recv_sem=sum_recv.at[stage, k, source],
            device_id=device(target),
            device_id_type=MESH,
        )

    def spread(group, k, value):
        buffer, _, me, size, _ = group
        buffer[k, me] = value
        for d in range(1, size):
            piece(group, k, me, d, (me + d) % size).start()

    def gather(group, k):
        buffer, _, me, size, _ = group
        for d in range(1, size):
            source = (me + d) % size
            piece(group, k, source, d, source).wait_recv()
        value = buffer[k, 0]
        for i in range(1, size):
            value = value + buffer[k, i]
        for d in range(1, size):
            piece(group, k, me, d, (me + d) % size).wait_send()
        return value

    def advance(stage, k):
        value = gather(groups[stage], k)
        if stage < 2:
            spread(groups[stage + 1], k, value)
        else:
            table[pl.ds(2 * BW * k, 2 * BW), :] = value

    for n in range(8):
        @pl.when(around[n][2])
        def _():
            edge(n).start()

    for b in range(BW):
        start(0, b)

    coef[...] = jnp.zeros((16, 128), jnp.float32)
    for i in range(3):
        for j in range(3):
            coef[3 * i + j : 3 * i + j + 1, 0:27] = stencil_ref[i, j : j + 1, :]
    copy = pltpu.make_async_copy(coef, coef_s, local_sem)
    copy.start()
    centre, half = spectrum(cos_ref, sin_ref, coef, scale_ref)
    inverse = 1.0 / half
    inv3 = inverse.reshape(1, 1, 1)
    cen3 = centre.reshape(1, 1, 1)
    sample = sample_ref[...]
    spot = sample >> 7
    lane = sample & 127
    px = jnp.where(spot >= 48, 1, 0)
    rest = spot - 48 * px
    py = (rest * 171) >> 9
    pc = rest - 3 * py
    mine = pc * 32 + px * 16 + py
    spots = lax.broadcasted_iota(jnp.int32, (96, 128), 0)
    chosen = jnp.where(spots == mine, 1.0, 0.0)
    mask[...] = chosen * np.float32(1.0 / np.sqrt(128.0))
    common = lax.broadcasted_iota(jnp.int32, (128, 128), 0) & lane
    common = common ^ (common >> 4)
    common = common ^ (common >> 2)
    common = common ^ (common >> 1)
    hadamard = (1 - 2 * (common & 1)).astype(jnp.float32)
    signs = jnp.concatenate([signs_ref[x, c] for c in range(3) for x in range(2)], axis=0)
    signs = (2 * signs - 1).astype(jnp.float32)
    picked = lax.dot_general(
        signs, chosen, (((0,), (0,)), ((), ())), precision=HIGH, preferred_element_type=jnp.float32
    )
    signed[...] = hadamard * picked

    def sketch(k):
        out = []
        for b in range(BW):
            block = v[k, b, :, OWN, ROW0 : ROW0 + 16, :].reshape(96, 128)
            spread_out = jnp.dot(block, signed[...], precision=HIGH, preferred_element_type=jnp.float32)
            out.append(jnp.sum(spread_out * mask[...], axis=0, keepdims=True))
        return out

    spread(groups[0], 0, jnp.concatenate([jnp.zeros((BW, 128), jnp.float32)] + sketch(0), axis=0))
    copy.wait()

    for n in range(8):
        @pl.when(around[n][2])
        def _():
            edge(7 - n).wait_recv()

    field = factor[...]
    alpha[...] = jnp.where(field > 0.0, field * (2.0 * inv3), 0.0)
    beta[...] = jnp.where(
        field > 0.0, -2.0 * cen3 * inv3, jnp.where(field == FIXED, 2.0 * (1.0 - cen3) * inv3, 0.0)
    )

    z_lane = lax.broadcasted_iota(jnp.int32, (1, 1, 128), 2)
    not_last = z_lane < 127
    not_first = z_lane > 0

    def apply(k, before, b, own, old, plane, row, height):
        total = [None, None, None]
        for dz in (-1, 1, 0):
            acc = list(total) if dz == 0 else [None, None, None]
            for dx in (-1, 0, 1):
                for dy in (-1, 0, 1):
                    offset = 9 * (dx + 1) + 3 * (dy + 1) + (dz + 1)
                    for j in range(3):
                        field = v[k, b, j, pl.ds(plane + dx, 2), pl.ds(row + dy, height), :]
                        for i in range(3):
                            term = coef_s[3 * i + j, offset] * field
                            acc[i] = term if acc[i] is None else acc[i] + term
            for i in range(3):
                if dz == -1:
                    total[i] = jnp.where(not_first, pltpu.roll(acc[i], 1, 2), 0.0)
                elif dz == 1:
                    total[i] = total[i] + jnp.where(not_last, pltpu.roll(acc[i], 127, 2), 0.0)
                else:
                    total[i] = acc[i]
        a = alpha[pl.ds(plane - 1, 2), row : row + height, :]
        d = beta[pl.ds(plane - 1, 2), row : row + height, :]
        for i in range(3):
            mid = v[k, b, i, pl.ds(plane, 2), row : row + height, :]
            value = a * total[i] + d * mid
            if own is not None:
                last = v[before, b, i, pl.ds(plane, 2), row : row + height, :]
                value = jnp.where(old, own * value, own * value - last)
            else:
                value = value - v[before, b, i, pl.ds(plane, 2), row : row + height, :]
            v[k + 1, b, i, pl.ds(plane, 2), row : row + height, :] = value

    def pair(t, carry):
        k = 2 * t
        start_of = k == 0
        own = jnp.where(start_of, jnp.float32(0.5), jnp.float32(1.0))
        before = jnp.maximum(k - 1, 0)

        def column(b, carry):
            arrive(k, b)

            def wide(side, carry):
                apply(k, before, b, own, start_of, 1 + 2 * side, ROW0 - 1, 24)
                return carry

            lax.fori_loop(0, 2, wide, 0)
            apply(k + 1, k, b, None, None, 2, ROW0, 16)

            @pl.when(t + 1 < PAIRS)
            def _():
                start(k + 2, b)

            @pl.when(b == 1)
            def _():
                advance(0, t)

            return carry

        lax.fori_loop(0, BW, column, 0)
        spread(groups[0], t + 1, jnp.concatenate(sketch(k + 1) + sketch(k + 2), axis=0))
        advance(1, t)

        @pl.when(t >= 1)
        def _():
            advance(2, t - 1)

        def drain(b, carry):
            sent(k, b)
            return carry

        lax.fori_loop(0, BW, drain, 0)
        return carry

    lax.fori_loop(0, PAIRS, pair, 0)
    for n in range(8):
        @pl.when(around[n][2])
        def _():
            edge(n).wait_send()

    advance(0, PAIRS)
    advance(2, PAIRS - 1)
    advance(1, PAIRS)
    advance(2, PAIRS)

    rows[0:BW] = least_squares(table[...], centre * inverse, half)
    copy = pltpu.make_async_copy(rows, weights, local_sem)
    copy.start()
    copy.wait()

    def combine(b, carry):
        for x in range(2):
            sol = jnp.zeros((3, 16, 128), jnp.float32)
            res = jnp.zeros((3, 16, 128), jnp.float32)
            for k in range(NV):
                for a in range(BW):
                    field = v[k, a, :, 2 + x, ROW0 : ROW0 + 16, :]
                    res = res + weights[b, BW * (k + 1) + a] * field
                    if k < STEPS:
                        sol = sol - weights[b, 64 + BW * (k + 1) + a] * field
            solution_ref[b, :, x] = sol
            residual_ref[b, :, x] = res
        return carry

    lax.fori_loop(0, BW, combine, 0)


def solution(mesh):
    n_gx, n_gy = mesh.shape["gx"], mesh.shape["gy"]
    n_z = 8 if n_gx % 8 == 0 else n_gx
    n_y = n_gx // n_z
    cosine, sine = phase_tables()

    def shards(right_side, stencil, class_scale, material, boundary, sign_bits, sample_rows):
        rhs = jnp.transpose(right_side, (0, 1, 3, 2, 4))
        signs = jnp.transpose(sign_bits, (0, 2, 1, 3))
        blocks = jnp.transpose(stencil, (1, 2, 0))
        vmem = pl.BlockSpec(memory_space=pltpu.VMEM)
        smem = pl.BlockSpec(memory_space=pltpu.SMEM)
        hbm = pl.BlockSpec(memory_space=pl.ANY)
        out = jax.ShapeDtypeStruct((BW, 3, 2, 16, 128), jnp.float32)
        most = max(n_gy, n_y, n_z)
        answer, residual = pl.pallas_call(
            lambda *refs: cycle_kernel(n_gx, n_gy, n_y, n_z, *refs),
            out_shape=(out, out),
            in_specs=[smem, hbm] + [vmem] * 7,
            out_specs=(vmem, vmem),
            scratch_shapes=[
                pltpu.VMEM((NV, BW, 3, 6, 32, 128), jnp.float32),
                pltpu.VMEM((4, 32, 128), jnp.float32),
                pltpu.VMEM((4, 32, 128), jnp.float32),
                pltpu.VMEM((4, 32, 128), jnp.float32),
                pltpu.VMEM((96, 128), jnp.float32),
                pltpu.VMEM((128, 128), jnp.float32),
                pltpu.VMEM((16, 128), jnp.float32),
                pltpu.SMEM((16, 128), jnp.float32),
                pltpu.VMEM((128, 128), jnp.float32),
                pltpu.VMEM((8, 128), jnp.float32),
                pltpu.SMEM((8, 128), jnp.float32),
                pltpu.VMEM((GROUPS, n_gy, 2 * BW, 128), jnp.float32),
                pltpu.VMEM((GROUPS, n_y, 2 * BW, 128), jnp.float32),
                pltpu.VMEM((GROUPS, n_z, 2 * BW, 128), jnp.float32),
                pltpu.SemaphoreType.DMA((PAIRS, BW, 8)),
                pltpu.SemaphoreType.DMA((PAIRS, BW, 8)),
                pltpu.SemaphoreType.DMA((8,)),
                pltpu.SemaphoreType.DMA((8,)),
                pltpu.SemaphoreType.DMA((3 * BW,)),
                pltpu.SemaphoreType.DMA((3, GROUPS, most)),
                pltpu.SemaphoreType.DMA((3, GROUPS, most)),
                pltpu.SemaphoreType.DMA,
            ],
            compiler_params=pltpu.CompilerParams(collective_id=0, has_side_effects=True),
            name="cycle",
        )(
            class_scale, rhs, blocks, material, boundary, signs, sample_rows.reshape(1, 128),
            cosine, sine,
        )
        back = lambda t: jnp.transpose(t, (2, 3, 0, 1, 4))
        return back(answer), back(residual)

    return jax.shard_map(
        shards,
        mesh=mesh,
        in_specs=(
            P("gx", "gy", None, None, None),
            P(),
            P(),
            P("gx", "gy", None),
            P("gx", "gy", None),
            P("gx", "gy", None, None),
            P("gx", "gy", None),
        ),
        out_specs=(P("gx", "gy", None, None, None), P("gx", "gy", None, None, None)),
        check_vma=False,
    )
```

```python
import numpy as np
import jax
import jax.numpy as jnp
from jax import lax
from jax.experimental import pallas as pl
from jax.experimental.pallas import tpu as pltpu
from jax.sharding import PartitionSpec as P

STEPS = 8
NCLASS = 8
NV = STEPS + 1
BW = 4
NROW = NV * BW
HIGH = lax.Precision.HIGHEST
MESH = pl.DeviceIdType.MESH

ROW0 = 8
OWN = slice(2, 4)
PAIRS = STEPS // 2
GROUPS = PAIRS + 1
FIXED = -1.0


def phase_tables():
    points = [
        (x * np.pi / 3, y * np.pi / 2, z * np.pi / 4)
        for x in range(4)
        for y in range(4)
        for z in range(8)
    ]
    offsets = [(o // 9 - 1, (o // 3) % 3 - 1, o % 3 - 1) for o in range(27)]
    phase = np.zeros((128, 128))
    phase[:27] = np.array(offsets) @ np.array(points).T
    keep = (np.arange(128) < 27)[:, None]
    return (np.cos(phase) * keep).astype(np.float32), (np.sin(phase) * keep).astype(np.float32)


def neighbours(n_gx, n_gy):
    gx, gy = lax.axis_index("gx"), lax.axis_index("gy")
    out = []
    for dx in (-1, 0, 1):
        for dy in (-1, 0, 1):
            if dx == 0 and dy == 0:
                continue
            ok = jnp.bool_(True)
            if dx < 0:
                ok = jnp.logical_and(ok, gx > 0)
            if dx > 0:
                ok = jnp.logical_and(ok, gx < n_gx - 1)
            if dy < 0:
                ok = jnp.logical_and(ok, gy > 0)
            if dy > 0:
                ok = jnp.logical_and(ok, gy < n_gy - 1)
            out.append((dx, dy, ok, {"gx": gx + dx, "gy": gy + dy}))
    return out


def spectrum(cos_ref, sin_ref, coef_ref, scale_ref):
    coef = coef_ref[...]
    re = jnp.dot(coef, cos_ref[...], precision=HIGH, preferred_element_type=jnp.float32)
    im = jnp.dot(coef, sin_ref[...], precision=HIGH, preferred_element_type=jnp.float32)

    def row(t, i, j):
        return t[3 * i + j : 3 * i + j + 1]

    low, high = None, None
    for i in range(3):
        off = jnp.zeros((1, 128), jnp.float32)
        for j in range(3):
            if j != i:
                a = 0.5 * (row(re, i, j) + row(re, j, i))
                b = 0.5 * (row(im, i, j) - row(im, j, i))
                off = off + jnp.sqrt(a * a + b * b)
        lo, hi = row(re, i, i) - off, row(re, i, i) + off
        low = lo if low is None else jnp.minimum(low, lo)
        high = hi if high is None else jnp.maximum(high, hi)
    low = jnp.min(low, axis=1, keepdims=True)
    high = jnp.max(high, axis=1, keepdims=True)
    smin = smax = scale_ref[0]
    for n in range(1, NCLASS):
        smin = jnp.minimum(smin, scale_ref[n])
        smax = jnp.maximum(smax, scale_ref[n])
    low = jnp.minimum(jnp.minimum(low * smin, low * smax), 1.0)
    high = jnp.maximum(high * smax, 1.0)
    span = high - low
    low, high = low + 0.04 * span, high - 0.2 * span
    centre = 0.5 * (low + high)
    half = jnp.maximum(0.5 * (high - low), 1e-3 * high)
    return centre, half


class LeastSquares:
    def __init__(self, table, ratio, half):
        self.ratio, self.half = ratio, half
        self.lane = lax.broadcasted_iota(jnp.int32, (BW, 128), 1)
        row = lax.broadcasted_iota(jnp.int32, (BW, 128), 0)
        none, one, mid = jnp.float32(0.0), jnp.float32(1.0), jnp.float32(0.5)
        self.rhs = table[BW : 2 * BW]
        self.up = jnp.where(self.lane < 2 * BW, none, jnp.where(self.lane < 3 * BW, one, mid))
        self.down = jnp.where(jnp.logical_and(self.lane >= BW, self.lane < NROW + BW), mid, none)
        self.last = jnp.where(self.lane == row + BW, one, none)
        scale = self.inverse_norm(self.rhs)
        self.u, self.p = self.rhs * scale, self.last * scale
        self.weight = jnp.zeros((1, 128), jnp.float32)
        self.square = jnp.zeros((1, 128), jnp.float32)
        self.along = jnp.zeros((BW, 128), jnp.float32)
        self.q, self.e, self.count = None, None, 0

    def inverse_norm(self, t):
        return lax.rsqrt(jnp.sum(t * t, axis=1, keepdims=True) + 1e-6)

    def images(self, table, blocks):
        images, coefs = [], []
        for k in blocks:
            p, u = self.p, self.u
            d = self.half * (self.ratio * p + self.up * pltpu.roll(p, BW, 1) + self.down * pltpu.roll(p, 128 - BW, 1))
            image = jnp.dot(d, table, precision=HIGH, preferred_element_type=jnp.float32)
            images.append(image)
            coefs.append(d + pltpu.roll(p, 64, 1))
            if k + 1 < STEPS:
                rest, prest = image, d
                for i in range(BW):
                    coupling = jnp.sum(image * u[i : i + 1], axis=1, keepdims=True)
                    rest = rest - coupling * u[i : i + 1]
                    prest = prest - coupling * p[i : i + 1]
                scale = self.inverse_norm(rest)
                self.u, self.p = rest * scale, prest * scale
        return images, coefs

    def orthogonalise(self, images, coefs):
        size = BW * len(images)
        new, enew = jnp.concatenate(images, axis=0), jnp.concatenate(coefs, axis=0)
        n = self.count
        if n:
            dots = lax.dot_general(
                new, self.q, (((1,), (1,)), ((), ())), precision=HIGH, preferred_element_type=jnp.float32
            )
            dots = dots * (self.weight * (2.0 - self.square))[:, :n]
            new = new - jnp.dot(dots, self.q, precision=HIGH, preferred_element_type=jnp.float32)
            enew = enew - jnp.dot(dots, self.e, precision=HIGH, preferred_element_type=jnp.float32)
        q = jnp.concatenate([new, self.rhs], axis=0)
        e = jnp.concatenate([enew, self.last], axis=0)
        rows = lax.broadcasted_iota(jnp.int32, (size + BW, 1), 0)
        lanes = lax.broadcasted_iota(jnp.int32, (1, 128), 1)
        is_rhs = rows >= size
        for j in range(size):
            pivot = q[j : j + 1]
            dots = jnp.sum(q * pivot, axis=1, keepdims=True)
            w = 1.0 / (dots[j : j + 1] + 1e-6)
            s = dots[j : j + 1] * w
            here = lanes == n + j
            self.weight = self.weight + jnp.where(here, w, 0.0)
            self.square = self.square + jnp.where(here, s, 0.0)
            part = jnp.where(rows > j, dots * w * jnp.where(is_rhs, jnp.float32(1.0), 2.0 - s), 0.0)
            self.along = self.along + jnp.where(here, part[size:], 0.0)
            q = q - part * pivot
            e = e - part * e[j : j + 1]
        self.rhs, self.last = q[size:], e[size:]
        if n:
            self.q = jnp.concatenate([self.q, q[:size]], axis=0)
            self.e = jnp.concatenate([self.e, e[:size]], axis=0)
        else:
            self.q, self.e = q[:size], e[:size]
        self.count = n + size

    def refined(self, table):
        n = self.count
        here = jnp.where(self.lane < NROW + BW, self.last, 0.0)
        left = jnp.dot(here, table, precision=HIGH, preferred_element_type=jnp.float32)
        dots = lax.dot_general(
            left, self.q, (((1,), (1,)), ((), ())), precision=HIGH, preferred_element_type=jnp.float32
        )
        change = dots * self.weight[:, :n] - self.along[:, :n] * (1.0 - self.square[:, :n])
        return self.last - jnp.dot(change, self.e, precision=HIGH, preferred_element_type=jnp.float32)


def cycle_kernel(
    n_gx, n_gy, n_y, n_z,
    scale_ref, rhs_ref, stencil_ref, material_ref, boundary_ref, signs_ref, sample_ref, cos_ref, sin_ref,
    solution_ref, residual_ref,
    v, factor, alpha, beta, mask, signed, coef, coef_s, table, part_a, part_b, part_c,
    send_sem, recv_sem, factor_send, factor_recv, load_sem, sum_send, sum_recv, local_sem,
):
    gx, gy = lax.axis_index("gx"), lax.axis_index("gy")
    around = neighbours(n_gx, n_gy)
    here_y, here_z = gx // n_z, gx % n_z

    groups = (
        (part_a, 0, gy, n_gy, lambda i: {"gx": gx, "gy": i}),
        (part_b, 1, here_y, n_y, lambda i: {"gx": i * n_z + here_z, "gy": gy}),
        (part_c, 2, here_z, n_z, lambda i: {"gx": here_y * n_z + i, "gy": gy}),
    )

    loads = []
    for b in range(BW):
        for c in range(3):
            copy = pltpu.make_async_copy(
                rhs_ref.at[:, :, c, b, :], v.at[0, b, c, pl.ds(2, 2), pl.ds(ROW0, 16), :], load_sem.at[3 * b + c]
            )
            copy.start()
            loads.append(copy)

    barrier = pltpu.get_barrier_semaphore()
    count = jnp.int32(0)
    for dx, dy, ok, device in around:
        count = count + jnp.where(ok, 1, 0)

        @pl.when(ok)
        def _():
            pl.semaphore_signal(barrier, inc=1, device_id=device, device_id_type=MESH)

    for _, _, me, size, device in groups:
        count = count + (size - 1)
        for d in range(1, size):
            pl.semaphore_signal(barrier, inc=1, device_id=device((me + d) % size), device_id_type=MESH)

    def clear(t, carry):
        k = 2 * t

        @pl.when(gx == 0)
        def _():
            v[k, :, :, 0:2] = jnp.zeros((BW, 3, 2, 32, 128), jnp.float32)

        @pl.when(gx == n_gx - 1)
        def _():
            v[k, :, :, 4:6] = jnp.zeros((BW, 3, 2, 32, 128), jnp.float32)

        @pl.when(gy == 0)
        def _():
            v[k, :, :, :, ROW0 - 2 : ROW0, :] = jnp.zeros((BW, 3, 6, 2, 128), jnp.float32)

        @pl.when(gy == n_gy - 1)
        def _():
            v[k, :, :, :, ROW0 + 16 : ROW0 + 18, :] = jnp.zeros((BW, 3, 6, 2, 128), jnp.float32)

        return carry

    lax.fori_loop(0, PAIRS, clear, 0)

    @pl.when(gx == 0)
    def _():
        factor[0] = jnp.zeros((32, 128), jnp.float32)

    @pl.when(gx == n_gx - 1)
    def _():
        factor[3] = jnp.zeros((32, 128), jnp.float32)

    @pl.when(gy == 0)
    def _():
        factor[:, ROW0 - 1 : ROW0, :] = jnp.zeros((4, 1, 128), jnp.float32)

    @pl.when(gy == n_gy - 1)
    def _():
        factor[:, ROW0 + 16 : ROW0 + 17, :] = jnp.zeros((4, 1, 128), jnp.float32)

    material = material_ref[...]
    scales = jnp.zeros((2, 16, 128), jnp.float32)
    for n in range(NCLASS):
        scales = jnp.where(material == n, scale_ref[n], scales)
    factor[1:3, ROW0 : ROW0 + 16, :] = jnp.where(boundary_ref[...] == 1, FIXED, scales)
    table[...] = jnp.zeros((128, 128), jnp.float32)
    for copy in loads:
        copy.wait()
    pl.semaphore_wait(barrier, count)

    def halo(k, b, n):
        dx, dy, ok, device = around[n]
        plane = {-1: 4, 0: 2, 1: 0}[dx]
        ys = {-1: (ROW0, 2, ROW0 + 16), 0: (ROW0, 16, ROW0), 1: (ROW0 + 14, 2, ROW0 - 2)}[dy]
        return pltpu.make_async_remote_copy(
            src_ref=v.at[k, b, :, pl.ds(2, 2), pl.ds(ys[0], ys[1]), :],
            dst_ref=v.at[k, b, :, pl.ds(plane, 2), pl.ds(ys[2], ys[1]), :],
            send_sem=send_sem.at[k // 2, b, n],
            recv_sem=recv_sem.at[k // 2, b, n],
            device_id=device,
            device_id_type=MESH,
        )

    def edge(n):
        dx, dy, ok, device = around[n]
        xs = {-1: (1, 1, 3), 0: (1, 2, 1), 1: (2, 1, 0)}[dx]
        ys = {-1: (ROW0, 1, ROW0 + 16), 0: (ROW0, 16, ROW0), 1: (ROW0 + 15, 1, ROW0 - 1)}[dy]
        return pltpu.make_async_remote_copy(
            src_ref=factor.at[pl.ds(xs[0], xs[1]), pl.ds(ys[0], ys[1]), :],
            dst_ref=factor.at[pl.ds(xs[2], xs[1]), pl.ds(ys[2], ys[1]), :],
            send_sem=factor_send.at[n],
            recv_sem=factor_recv.at[n],
            device_id=device,
            device_id_type=MESH,
        )

    def start(k, b):
        for n in range(8):
            @pl.when(around[n][2])
            def _():
                halo(k, b, n).start()

    def arrive(k, b):
        for n in range(8):
            @pl.when(around[n][2])
            def _():
                halo(k, b, 7 - n).wait_recv()

    def sent(k, b):
        for n in range(8):
            @pl.when(around[n][2])
            def _():
                halo(k, b, n).wait_send()

    def piece(group, k, source, d, target):
        buffer, stage, _, _, device = group
        return pltpu.make_async_remote_copy(
            src_ref=buffer.at[k, source],
            dst_ref=buffer.at[k, source],
            send_sem=sum_send.at[stage, k, d],
            recv_sem=sum_recv.at[stage, k, source],
            device_id=device(target),
            device_id_type=MESH,
        )

    def spread(group, k, value):
        buffer, _, me, size, _ = group
        buffer[k, me] = value
        for d in range(1, size):
            piece(group, k, me, d, (me + d) % size).start()

    def gather(group, k):
        buffer, _, me, size, _ = group
        for d in range(1, size):
            source = (me + d) % size
            piece(group, k, source, d, source).wait_recv()
        value = buffer[k, 0]
        for i in range(1, size):
            value = value + buffer[k, i]
        for d in range(1, size):
            piece(group, k, me, d, (me + d) % size).wait_send()
        return value

    def advance(stage, k):
        value = gather(groups[stage], k)
        if stage < 2:
            spread(groups[stage + 1], k, value)
        else:
            table[pl.ds(2 * BW * k, 2 * BW), :] = value

    for n in range(8):
        @pl.when(around[n][2])
        def _():
            edge(n).start()

    for b in range(BW):
        start(0, b)

    coef[...] = jnp.zeros((16, 128), jnp.float32)
    for i in range(3):
        for j in range(3):
            coef[3 * i + j : 3 * i + j + 1, 0:27] = stencil_ref[i, j : j + 1, :]
    copy = pltpu.make_async_copy(coef, coef_s, local_sem)
    copy.start()
    centre, half = spectrum(cos_ref, sin_ref, coef, scale_ref)
    inverse = 1.0 / half
    inv3 = inverse.reshape(1, 1, 1)
    cen3 = centre.reshape(1, 1, 1)
    sample = sample_ref[...]
    spot = sample >> 7
    lane = sample & 127
    px = jnp.where(spot >= 48, 1, 0)
    rest = spot - 48 * px
    py = (rest * 171) >> 9
    pc = rest - 3 * py
    mine = pc * 32 + px * 16 + py
    spots = lax.broadcasted_iota(jnp.int32, (96, 128), 0)
    chosen = jnp.where(spots == mine, 1.0, 0.0)
    mask[...] = chosen * np.float32(1.0 / np.sqrt(128.0))
    common = lax.broadcasted_iota(jnp.int32, (128, 128), 0) & lane
    common = common ^ (common >> 4)
    common = common ^ (common >> 2)
    common = common ^ (common >> 1)
    hadamard = (1 - 2 * (common & 1)).astype(jnp.float32)
    signs = jnp.concatenate([signs_ref[x, c] for c in range(3) for x in range(2)], axis=0)
    signs = (2 * signs - 1).astype(jnp.float32)
    picked = lax.dot_general(
        signs, chosen, (((0,), (0,)), ((), ())), precision=HIGH, preferred_element_type=jnp.float32
    )
    signed[...] = hadamard * picked

    def sketch(k):
        out = []
        for b in range(BW):
            block = v[k, b, :, OWN, ROW0 : ROW0 + 16, :].reshape(96, 128)
            spread_out = jnp.dot(block, signed[...], precision=HIGH, preferred_element_type=jnp.float32)
            out.append(jnp.sum(spread_out * mask[...], axis=0, keepdims=True))
        return out

    spread(groups[0], 0, jnp.concatenate([jnp.zeros((BW, 128), jnp.float32)] + sketch(0), axis=0))
    copy.wait()

    for n in range(8):
        @pl.when(around[n][2])
        def _():
            edge(7 - n).wait_recv()

    field = factor[...]
    alpha[...] = jnp.where(field > 0.0, field * (2.0 * inv3), 0.0)
    beta[...] = jnp.where(
        field > 0.0, -2.0 * cen3 * inv3, jnp.where(field == FIXED, 2.0 * (1.0 - cen3) * inv3, 0.0)
    )

    z_lane = lax.broadcasted_iota(jnp.int32, (1, 1, 128), 2)
    not_last = z_lane < 127
    not_first = z_lane > 0

    def apply(k, before, b, own, old, plane, row, height):
        total = [None, None, None]
        for dz in (-1, 1, 0):
            acc = list(total) if dz == 0 else [None, None, None]
            for dx in (-1, 0, 1):
                for dy in (-1, 0, 1):
                    offset = 9 * (dx + 1) + 3 * (dy + 1) + (dz + 1)
                    for j in range(3):
                        field = v[k, b, j, pl.ds(plane + dx, 2), pl.ds(row + dy, height), :]
                        for i in range(3):
                            term = coef_s[3 * i + j, offset] * field
                            acc[i] = term if acc[i] is None else acc[i] + term
            for i in range(3):
                if dz == -1:
                    total[i] = jnp.where(not_first, pltpu.roll(acc[i], 1, 2), 0.0)
                elif dz == 1:
                    total[i] = total[i] + jnp.where(not_last, pltpu.roll(acc[i], 127, 2), 0.0)
                else:
                    total[i] = acc[i]
        a = alpha[pl.ds(plane - 1, 2), row : row + height, :]
        d = beta[pl.ds(plane - 1, 2), row : row + height, :]
        for i in range(3):
            mid = v[k, b, i, pl.ds(plane, 2), row : row + height, :]
            value = a * total[i] + d * mid
            if own is not None:
                last = v[before, b, i, pl.ds(plane, 2), row : row + height, :]
                value = jnp.where(old, own * value, own * value - last)
            else:
                value = value - v[before, b, i, pl.ds(plane, 2), row : row + height, :]
            v[k + 1, b, i, pl.ds(plane, 2), row : row + height, :] = value

    def pair(t, carry):
        k = 2 * t
        start_of = k == 0
        own = jnp.where(start_of, jnp.float32(0.5), jnp.float32(1.0))
        before = jnp.maximum(k - 1, 0)

        def column(b, carry):
            arrive(k, b)

            def wide(side, carry):
                apply(k, before, b, own, start_of, 1 + 2 * side, ROW0 - 1, 24)
                return carry

            lax.fori_loop(0, 2, wide, 0)
            apply(k + 1, k, b, None, None, 2, ROW0, 16)

            @pl.when(t + 1 < PAIRS)
            def _():
                start(k + 2, b)

            @pl.when(b == 1)
            def _():
                advance(0, t)

            return carry

        lax.fori_loop(0, BW, column, 0)
        spread(groups[0], t + 1, jnp.concatenate(sketch(k + 1) + sketch(k + 2), axis=0))
        advance(1, t)

        @pl.when(t >= 1)
        def _():
            advance(2, t - 1)

        def drain(b, carry):
            sent(k, b)
            return carry

        lax.fori_loop(0, BW, drain, 0)
        return carry

    lax.fori_loop(0, PAIRS, pair, 0)
    for n in range(8):
        @pl.when(around[n][2])
        def _():
            edge(n).wait_send()

    least = LeastSquares(table[...], centre * inverse, half)
    found = least.images(table[...], (0, 1, 2, 3))
    advance(0, PAIRS)
    least.orthogonalise(*found)
    advance(2, PAIRS - 1)
    advance(1, PAIRS)
    least.orthogonalise(*least.images(table[...], (4, 5)))
    advance(2, PAIRS)
    least.orthogonalise(*least.images(table[...], (6, 7)))
    last = least.refined(table[...])

    for b in range(BW):

        def weight(lane):
            return jnp.broadcast_to(last[b : b + 1, lane : lane + 1], (16, 128))[None]

        sol = [jnp.zeros((3, 16, 128), jnp.float32)] * 2
        res = [jnp.zeros((3, 16, 128), jnp.float32)] * 2
        for k in range(NV):
            for a in range(BW):
                spot = BW * (k + 1) + a
                for x in range(2):
                    field = v[k, a, :, 2 + x, ROW0 : ROW0 + 16, :]
                    res[x] = res[x] + weight(spot) * field
                    if k < STEPS:
                        sol[x] = sol[x] - weight(64 + spot) * field
        for x in range(2):
            solution_ref[b, :, x] = sol[x]
            residual_ref[b, :, x] = res[x]


def solution(mesh):
    n_gx, n_gy = mesh.shape["gx"], mesh.shape["gy"]
    n_z = 8 if n_gx % 8 == 0 else n_gx
    n_y = n_gx // n_z
    cosine, sine = phase_tables()

    def shards(right_side, stencil, class_scale, material, boundary, sign_bits, sample_rows):
        rhs = jnp.transpose(right_side, (0, 1, 3, 2, 4))
        signs = jnp.transpose(sign_bits, (0, 2, 1, 3))
        blocks = jnp.transpose(stencil, (1, 2, 0))
        vmem = pl.BlockSpec(memory_space=pltpu.VMEM)
        smem = pl.BlockSpec(memory_space=pltpu.SMEM)
        hbm = pl.BlockSpec(memory_space=pl.ANY)
        out = pltpu.VMEM((BW, 3, 2, 16, 128), jnp.float32)
        most = max(n_gy, n_y, n_z)
        answer, residual = pl.pallas_call(
            lambda *refs: cycle_kernel(n_gx, n_gy, n_y, n_z, *refs),
            out_shape=(out, out),
            in_specs=[smem, hbm] + [vmem] * 7,
            out_specs=(vmem, vmem),
            scratch_shapes=[
                pltpu.VMEM((NV, BW, 3, 6, 32, 128), jnp.float32),
                pltpu.VMEM((4, 32, 128), jnp.float32),
                pltpu.VMEM((4, 32, 128), jnp.float32),
                pltpu.VMEM((4, 32, 128), jnp.float32),
                pltpu.VMEM((96, 128), jnp.float32),
                pltpu.VMEM((128, 128), jnp.float32),
                pltpu.VMEM((16, 128), jnp.float32),
                pltpu.SMEM((16, 128), jnp.float32),
                pltpu.VMEM((128, 128), jnp.float32),
                pltpu.VMEM((GROUPS, n_gy, 2 * BW, 128), jnp.float32),
                pltpu.VMEM((GROUPS, n_y, 2 * BW, 128), jnp.float32),
                pltpu.VMEM((GROUPS, n_z, 2 * BW, 128), jnp.float32),
                pltpu.SemaphoreType.DMA((PAIRS, BW, 8)),
                pltpu.SemaphoreType.DMA((PAIRS, BW, 8)),
                pltpu.SemaphoreType.DMA((8,)),
                pltpu.SemaphoreType.DMA((8,)),
                pltpu.SemaphoreType.DMA((3 * BW,)),
                pltpu.SemaphoreType.DMA((3, GROUPS, most)),
                pltpu.SemaphoreType.DMA((3, GROUPS, most)),
                pltpu.SemaphoreType.DMA,
            ],
            compiler_params=pltpu.CompilerParams(collective_id=0, has_side_effects=True),
            name="cycle",
        )(
            class_scale, rhs, blocks, material, boundary, signs, sample_rows.reshape(1, 128),
            cosine, sine,
        )
        back = lambda t: jnp.transpose(t, (2, 3, 0, 1, 4))
        return back(answer), back(residual)

    return jax.shard_map(
        shards,
        mesh=mesh,
        in_specs=(
            P("gx", "gy", None, None, None),
            P(),
            P(),
            P("gx", "gy", None),
            P("gx", "gy", None),
            P("gx", "gy", None, None),
            P("gx", "gy", None),
        ),
        out_specs=(P("gx", "gy", None, None, None), P("gx", "gy", None, None, None)),
        check_vma=False,
    )
```

```python
import numpy as np
import jax
import jax.numpy as jnp
from jax import lax
from jax.experimental import pallas as pl
from jax.experimental.pallas import tpu as pltpu
from jax.sharding import PartitionSpec as P

STEPS = 8
NCLASS = 8
NV = STEPS + 1
BW = 4
NROW = NV * BW
HIGH = lax.Precision.HIGHEST
MESH = pl.DeviceIdType.MESH

ROW0 = 8
OWN = slice(2, 4)
PAIRS = STEPS // 2
GROUPS = PAIRS + 1
FIXED = -1.0


def phase_tables():
    points = [
        (x * np.pi / 3, y * np.pi / 2, z * np.pi / 4)
        for x in range(4)
        for y in range(4)
        for z in range(8)
    ]
    offsets = [(o // 9 - 1, (o // 3) % 3 - 1, o % 3 - 1) for o in range(27)]
    phase = np.zeros((128, 128))
    phase[:27] = np.array(offsets) @ np.array(points).T
    keep = (np.arange(128) < 27)[:, None]
    return (np.cos(phase) * keep).astype(np.float32), (np.sin(phase) * keep).astype(np.float32)


def neighbours(n_gx, n_gy):
    gx, gy = lax.axis_index("gx"), lax.axis_index("gy")
    out = []
    for dx in (-1, 0, 1):
        for dy in (-1, 0, 1):
            if dx == 0 and dy == 0:
                continue
            ok = jnp.bool_(True)
            if dx < 0:
                ok = jnp.logical_and(ok, gx > 0)
            if dx > 0:
                ok = jnp.logical_and(ok, gx < n_gx - 1)
            if dy < 0:
                ok = jnp.logical_and(ok, gy > 0)
            if dy > 0:
                ok = jnp.logical_and(ok, gy < n_gy - 1)
            out.append((dx, dy, ok, {"gx": gx + dx, "gy": gy + dy}))
    return out


def spectrum(cos_ref, sin_ref, coef_ref, scale_ref):
    coef = coef_ref[...]
    re = jnp.dot(coef, cos_ref[...], precision=HIGH, preferred_element_type=jnp.float32)
    im = jnp.dot(coef, sin_ref[...], precision=HIGH, preferred_element_type=jnp.float32)

    def row(t, i, j):
        return t[3 * i + j : 3 * i + j + 1]

    low, high = None, None
    for i in range(3):
        off = jnp.zeros((1, 128), jnp.float32)
        for j in range(3):
            if j != i:
                a = 0.5 * (row(re, i, j) + row(re, j, i))
                b = 0.5 * (row(im, i, j) - row(im, j, i))
                off = off + jnp.sqrt(a * a + b * b)
        lo, hi = row(re, i, i) - off, row(re, i, i) + off
        low = lo if low is None else jnp.minimum(low, lo)
        high = hi if high is None else jnp.maximum(high, hi)
    low = jnp.min(low, axis=1, keepdims=True)
    high = jnp.max(high, axis=1, keepdims=True)
    smin = smax = scale_ref[0]
    for n in range(1, NCLASS):
        smin = jnp.minimum(smin, scale_ref[n])
        smax = jnp.maximum(smax, scale_ref[n])
    low = jnp.minimum(jnp.minimum(low * smin, low * smax), 1.0)
    high = jnp.maximum(high * smax, 1.0)
    span = high - low
    low, high = low + 0.04 * span, high - 0.2 * span
    centre = 0.5 * (low + high)
    half = jnp.maximum(0.5 * (high - low), 1e-3 * high)
    return centre, half


class LeastSquares:
    def __init__(self, table, ratio, half):
        self.ratio, self.half = ratio, half
        self.lane = lax.broadcasted_iota(jnp.int32, (BW, 128), 1)
        row = lax.broadcasted_iota(jnp.int32, (BW, 128), 0)
        none, one, mid = jnp.float32(0.0), jnp.float32(1.0), jnp.float32(0.5)
        self.rhs = table[BW : 2 * BW]
        self.up = jnp.where(self.lane < 2 * BW, none, jnp.where(self.lane < 3 * BW, one, mid))
        self.down = jnp.where(jnp.logical_and(self.lane >= BW, self.lane < NROW + BW), mid, none)
        self.last = jnp.where(self.lane == row + BW, one, none)
        scale = self.inverse_norm(self.rhs)
        self.u, self.p = self.rhs * scale, self.last * scale
        self.weight = jnp.zeros((1, 128), jnp.float32)
        self.square = jnp.zeros((1, 128), jnp.float32)
        self.along = jnp.zeros((BW, 128), jnp.float32)
        self.q, self.e, self.count = None, None, 0

    def inverse_norm(self, t):
        return lax.rsqrt(jnp.sum(t * t, axis=1, keepdims=True) + 1e-6)

    def images(self, table, blocks):
        images, coefs = [], []
        for k in blocks:
            p, u = self.p, self.u
            d = self.half * (self.ratio * p + self.up * pltpu.roll(p, BW, 1) + self.down * pltpu.roll(p, 128 - BW, 1))
            image = jnp.dot(d, table, precision=HIGH, preferred_element_type=jnp.float32)
            images.append(image)
            coefs.append(d + pltpu.roll(p, 64, 1))
            if k + 1 < STEPS:
                rest, prest = image, d
                for i in range(BW):
                    coupling = jnp.sum(image * u[i : i + 1], axis=1, keepdims=True)
                    rest = rest - coupling * u[i : i + 1]
                    prest = prest - coupling * p[i : i + 1]
                scale = self.inverse_norm(rest)
                self.u, self.p = rest * scale, prest * scale
        return images, coefs

    def orthogonalise(self, images, coefs):
        size = BW * len(images)
        new, enew = jnp.concatenate(images, axis=0), jnp.concatenate(coefs, axis=0)
        n = self.count
        if n:
            dots = lax.dot_general(
                new, self.q, (((1,), (1,)), ((), ())), precision=HIGH, preferred_element_type=jnp.float32
            )
            dots = dots * (self.weight * (2.0 - self.square))[:, :n]
            new = new - jnp.dot(dots, self.q, precision=HIGH, preferred_element_type=jnp.float32)
            enew = enew - jnp.dot(dots, self.e, precision=HIGH, preferred_element_type=jnp.float32)
        q = jnp.concatenate([new, self.rhs], axis=0)
        e = jnp.concatenate([enew, self.last], axis=0)
        rows = lax.broadcasted_iota(jnp.int32, (size + BW, 1), 0)
        lanes = lax.broadcasted_iota(jnp.int32, (1, 128), 1)
        is_rhs = rows >= size
        for j in range(size):
            pivot = q[j : j + 1]
            dots = jnp.sum(q * pivot, axis=1, keepdims=True)
            w = 1.0 / (dots[j : j + 1] + 1e-6)
            s = dots[j : j + 1] * w
            here = lanes == n + j
            self.weight = self.weight + jnp.where(here, w, 0.0)
            self.square = self.square + jnp.where(here, s, 0.0)
            part = jnp.where(rows > j, dots * w * jnp.where(is_rhs, jnp.float32(1.0), 2.0 - s), 0.0)
            self.along = self.along + jnp.where(here, part[size:], 0.0)
            q = q - part * pivot
            e = e - part * e[j : j + 1]
        self.rhs, self.last = q[size:], e[size:]
        if n:
            self.q = jnp.concatenate([self.q, q[:size]], axis=0)
            self.e = jnp.concatenate([self.e, e[:size]], axis=0)
        else:
            self.q, self.e = q[:size], e[:size]
        self.count = n + size

    def refined(self, table):
        n = self.count
        here = jnp.where(self.lane < NROW + BW, self.last, 0.0)
        left = jnp.dot(here, table, precision=HIGH, preferred_element_type=jnp.float32)
        dots = lax.dot_general(
            left, self.q, (((1,), (1,)), ((), ())), precision=HIGH, preferred_element_type=jnp.float32
        )
        change = dots * self.weight[:, :n] - self.along[:, :n] * (1.0 - self.square[:, :n])
        return self.last - jnp.dot(change, self.e, precision=HIGH, preferred_element_type=jnp.float32)


def cycle_kernel(
    n_gx, n_gy, n_y, n_z,
    scale_ref, rhs_ref, stencil_ref, material_ref, boundary_ref, signs_ref, sample_ref, cos_ref, sin_ref,
    solution_ref, residual_ref,
    v, factor, alpha, beta, mask, signed, coef, coef_s, table, part_a, part_b, part_c,
    send_sem, recv_sem, factor_send, factor_recv, load_sem, sum_send, sum_recv, local_sem,
):
    gx, gy = lax.axis_index("gx"), lax.axis_index("gy")
    around = neighbours(n_gx, n_gy)
    here_y, here_z = gx // n_z, gx % n_z

    groups = (
        (part_a, 0, gy, n_gy, lambda i: {"gx": gx, "gy": i}),
        (part_b, 1, here_y, n_y, lambda i: {"gx": i * n_z + here_z, "gy": gy}),
        (part_c, 2, here_z, n_z, lambda i: {"gx": here_y * n_z + i, "gy": gy}),
    )

    loads = []
    for b in range(BW):
        for c in range(3):
            copy = pltpu.make_async_copy(
                rhs_ref.at[:, :, c, b, :], v.at[0, b, c, pl.ds(2, 2), pl.ds(ROW0, 16), :], load_sem.at[3 * b + c]
            )
            copy.start()
            loads.append(copy)

    barrier = pltpu.get_barrier_semaphore()
    count = jnp.int32(0)
    for _, _, me, size, device in reversed(groups):
        count = count + (size - 1)
        for d in range(1, size):
            pl.semaphore_signal(barrier, inc=1, device_id=device((me + d) % size), device_id_type=MESH)

    for dx, dy, ok, device in around:
        count = count + jnp.where(ok, 1, 0)

        @pl.when(ok)
        def _():
            pl.semaphore_signal(barrier, inc=1, device_id=device, device_id_type=MESH)

    def clear(t, carry):
        k = 2 * t

        @pl.when(gx == 0)
        def _():
            v[k, :, :, 0:2] = jnp.zeros((BW, 3, 2, 32, 128), jnp.float32)

        @pl.when(gx == n_gx - 1)
        def _():
            v[k, :, :, 4:6] = jnp.zeros((BW, 3, 2, 32, 128), jnp.float32)

        @pl.when(gy == 0)
        def _():
            v[k, :, :, :, ROW0 - 2 : ROW0, :] = jnp.zeros((BW, 3, 6, 2, 128), jnp.float32)

        @pl.when(gy == n_gy - 1)
        def _():
            v[k, :, :, :, ROW0 + 16 : ROW0 + 18, :] = jnp.zeros((BW, 3, 6, 2, 128), jnp.float32)

        return carry

    lax.fori_loop(0, PAIRS, clear, 0)

    @pl.when(gx == 0)
    def _():
        factor[0] = jnp.zeros((32, 128), jnp.float32)

    @pl.when(gx == n_gx - 1)
    def _():
        factor[3] = jnp.zeros((32, 128), jnp.float32)

    @pl.when(gy == 0)
    def _():
        factor[:, ROW0 - 1 : ROW0, :] = jnp.zeros((4, 1, 128), jnp.float32)

    @pl.when(gy == n_gy - 1)
    def _():
        factor[:, ROW0 + 16 : ROW0 + 17, :] = jnp.zeros((4, 1, 128), jnp.float32)

    material = material_ref[...]
    scales = jnp.zeros((2, 16, 128), jnp.float32)
    for n in range(NCLASS):
        scales = jnp.where(material == n, scale_ref[n], scales)
    factor[1:3, ROW0 : ROW0 + 16, :] = jnp.where(boundary_ref[...] == 1, FIXED, scales)
    table[...] = jnp.zeros((128, 128), jnp.float32)
    for copy in loads:
        copy.wait()
    pl.semaphore_wait(barrier, count)

    def halo(k, b, n):
        dx, dy, ok, device = around[n]
        plane = {-1: 4, 0: 2, 1: 0}[dx]
        ys = {-1: (ROW0, 2, ROW0 + 16), 0: (ROW0, 16, ROW0), 1: (ROW0 + 14, 2, ROW0 - 2)}[dy]
        return pltpu.make_async_remote_copy(
            src_ref=v.at[k, b, :, pl.ds(2, 2), pl.ds(ys[0], ys[1]), :],
            dst_ref=v.at[k, b, :, pl.ds(plane, 2), pl.ds(ys[2], ys[1]), :],
            send_sem=send_sem.at[k // 2, b, n],
            recv_sem=recv_sem.at[k // 2, b, n],
            device_id=device,
            device_id_type=MESH,
        )

    def edge(n):
        dx, dy, ok, device = around[n]
        xs = {-1: (1, 1, 3), 0: (1, 2, 1), 1: (2, 1, 0)}[dx]
        ys = {-1: (ROW0, 1, ROW0 + 16), 0: (ROW0, 16, ROW0), 1: (ROW0 + 15, 1, ROW0 - 1)}[dy]
        return pltpu.make_async_remote_copy(
            src_ref=factor.at[pl.ds(xs[0], xs[1]), pl.ds(ys[0], ys[1]), :],
            dst_ref=factor.at[pl.ds(xs[2], xs[1]), pl.ds(ys[2], ys[1]), :],
            send_sem=factor_send.at[n],
            recv_sem=factor_recv.at[n],
            device_id=device,
            device_id_type=MESH,
        )

    def start(k, b):
        for n in range(8):
            @pl.when(around[n][2])
            def _():
                halo(k, b, n).start()

    def arrive(k, b):
        for n in range(8):
            @pl.when(around[n][2])
            def _():
                halo(k, b, 7 - n).wait_recv()

    def sent(k, b):
        for n in range(8):
            @pl.when(around[n][2])
            def _():
                halo(k, b, n).wait_send()

    def piece(group, k, source, d, target):
        buffer, stage, _, _, device = group
        return pltpu.make_async_remote_copy(
            src_ref=buffer.at[k, source],
            dst_ref=buffer.at[k, source],
            send_sem=sum_send.at[stage, k, d],
            recv_sem=sum_recv.at[stage, k, source],
            device_id=device(target),
            device_id_type=MESH,
        )

    def spread(group, k, value):
        buffer, _, me, size, _ = group
        buffer[k, me] = value
        for d in range(1, size):
            piece(group, k, me, d, (me + d) % size).start()

    def gather(group, k):
        buffer, _, me, size, _ = group
        for d in range(1, size):
            source = (me + d) % size
            piece(group, k, source, d, source).wait_recv()
        value = buffer[k, 0]
        for i in range(1, size):
            value = value + buffer[k, i]
        for d in range(1, size):
            piece(group, k, me, d, (me + d) % size).wait_send()
        return value

    def advance(stage, k):
        value = gather(groups[stage], k)
        if stage < 2:
            spread(groups[stage + 1], k, value)
        else:
            table[pl.ds(2 * BW * k, 2 * BW), :] = value

    for n in range(8):
        @pl.when(around[n][2])
        def _():
            edge(n).start()

    for b in range(BW):
        start(0, b)

    coef[...] = jnp.zeros((16, 128), jnp.float32)
    for i in range(3):
        for j in range(3):
            coef[3 * i + j : 3 * i + j + 1, 0:27] = stencil_ref[i, j : j + 1, :]
    copy = pltpu.make_async_copy(coef, coef_s, local_sem)
    copy.start()
    centre, half = spectrum(cos_ref, sin_ref, coef, scale_ref)
    inverse = 1.0 / half
    inv3 = inverse.reshape(1, 1, 1)
    cen3 = centre.reshape(1, 1, 1)
    sample = sample_ref[...]
    spot = sample >> 7
    lane = sample & 127
    px = jnp.where(spot >= 48, 1, 0)
    rest = spot - 48 * px
    py = (rest * 171) >> 9
    pc = rest - 3 * py
    mine = pc * 32 + px * 16 + py
    spots = lax.broadcasted_iota(jnp.int32, (96, 128), 0)
    chosen = jnp.where(spots == mine, 1.0, 0.0)
    mask[...] = chosen * np.float32(1.0 / np.sqrt(128.0))
    common = lax.broadcasted_iota(jnp.int32, (128, 128), 0) & lane
    common = common ^ (common >> 4)
    common = common ^ (common >> 2)
    common = common ^ (common >> 1)
    hadamard = (1 - 2 * (common & 1)).astype(jnp.float32)
    signs = jnp.concatenate([signs_ref[x, c] for c in range(3) for x in range(2)], axis=0)
    signs = (2 * signs - 1).astype(jnp.float32)
    picked = lax.dot_general(
        signs, chosen, (((0,), (0,)), ((), ())), precision=HIGH, preferred_element_type=jnp.float32
    )
    signed[...] = (hadamard * picked).astype(jnp.bfloat16)

    def sketch(k):
        block = v[k, :, :, OWN, ROW0 : ROW0 + 16, :].reshape(96 * BW, 128)
        parts = []
        for _ in range(3):
            part = block.astype(jnp.bfloat16)
            parts.append(part)
            block = block - part.astype(jnp.float32)
        found = [jnp.dot(part, signed[...], preferred_element_type=jnp.float32) for part in reversed(parts)]
        found = (found[0] + found[1]) + found[2]
        picked = mask[...]
        return [
            jnp.sum(found[96 * b : 96 * (b + 1)] * picked, axis=0, keepdims=True) for b in range(BW)
        ]

    spread(groups[0], 0, jnp.concatenate([jnp.zeros((BW, 128), jnp.float32)] + sketch(0), axis=0))
    copy.wait()

    for n in range(8):
        @pl.when(around[n][2])
        def _():
            edge(7 - n).wait_recv()

    field = factor[...]
    alpha[...] = jnp.where(field > 0.0, field * (2.0 * inv3), 0.0)
    beta[...] = jnp.where(
        field > 0.0, -2.0 * cen3 * inv3, jnp.where(field == FIXED, 2.0 * (1.0 - cen3) * inv3, 0.0)
    )

    z_lane = lax.broadcasted_iota(jnp.int32, (1, 1, 128), 2)
    not_last = z_lane < 127
    not_first = z_lane > 0

    def apply(k, before, b, own, old, plane, row, height):
        total = [None, None, None]
        for dz in (-1, 1, 0):
            acc = list(total) if dz == 0 else [None, None, None]
            for dx in (-1, 0, 1):
                for dy in (-1, 0, 1):
                    offset = 9 * (dx + 1) + 3 * (dy + 1) + (dz + 1)
                    for j in range(3):
                        field = v[k, b, j, pl.ds(plane + dx, 2), pl.ds(row + dy, height), :]
                        for i in range(3):
                            term = coef_s[3 * i + j, offset] * field
                            acc[i] = term if acc[i] is None else acc[i] + term
            for i in range(3):
                if dz == -1:
                    total[i] = jnp.where(not_first, pltpu.roll(acc[i], 1, 2), 0.0)
                elif dz == 1:
                    total[i] = total[i] + jnp.where(not_last, pltpu.roll(acc[i], 127, 2), 0.0)
                else:
                    total[i] = acc[i]
        a = alpha[pl.ds(plane - 1, 2), row : row + height, :]
        d = beta[pl.ds(plane - 1, 2), row : row + height, :]
        for i in range(3):
            mid = v[k, b, i, pl.ds(plane, 2), row : row + height, :]
            value = a * total[i] + d * mid
            if own is not None:
                last = v[before, b, i, pl.ds(plane, 2), row : row + height, :]
                value = jnp.where(old, own * value, own * value - last)
            else:
                value = value - v[before, b, i, pl.ds(plane, 2), row : row + height, :]
            v[k + 1, b, i, pl.ds(plane, 2), row : row + height, :] = value

    def pair(t, carry):
        k = 2 * t
        start_of = k == 0
        own = jnp.where(start_of, jnp.float32(0.5), jnp.float32(1.0))
        before = jnp.maximum(k - 1, 0)

        def column(b, carry):
            arrive(k, b)

            def wide(side, carry):
                apply(k, before, b, own, start_of, 1 + 2 * side, ROW0 - 1, 24)
                return carry

            lax.fori_loop(0, 2, wide, 0)
            apply(k + 1, k, b, None, None, 2, ROW0, 16)

            @pl.when(t + 1 < PAIRS)
            def _():
                start(k + 2, b)

            @pl.when(jnp.logical_and(b == 1, t >= 1))
            def _():
                advance(1, t - 1)

            @pl.when(b == 3)
            def _():
                advance(0, t)

            return carry

        lax.fori_loop(0, BW, column, 0)
        spread(groups[0], t + 1, jnp.concatenate(sketch(k + 1) + sketch(k + 2), axis=0))

        @pl.when(t >= 2)
        def _():
            advance(2, t - 2)

        def drain(b, carry):
            sent(k, b)
            return carry

        lax.fori_loop(0, BW, drain, 0)
        return carry

    lax.fori_loop(0, PAIRS, pair, 0)
    for n in range(8):
        @pl.when(around[n][2])
        def _():
            edge(n).wait_send()

    advance(2, PAIRS - 2)
    least = LeastSquares(table[...], centre * inverse, half)
    found = least.images(table[...], (0, 1, 2, 3))
    advance(0, PAIRS)
    advance(1, PAIRS - 1)
    least.orthogonalise(*found)
    advance(1, PAIRS)
    advance(2, PAIRS - 1)
    least.orthogonalise(*least.images(table[...], (4, 5)))
    advance(2, PAIRS)
    least.orthogonalise(*least.images(table[...], (6, 7)))
    last = least.refined(table[...])

    for b in range(BW):

        def weight(lane):
            return jnp.broadcast_to(last[b : b + 1, lane : lane + 1], (16, 128))[None]

        sol = [jnp.zeros((3, 16, 128), jnp.float32)] * 2
        res = [jnp.zeros((3, 16, 128), jnp.float32)] * 2
        for k in range(NV):
            for a in range(BW):
                spot = BW * (k + 1) + a
                for x in range(2):
                    field = v[k, a, :, 2 + x, ROW0 : ROW0 + 16, :]
                    res[x] = res[x] + weight(spot) * field
                    if k < STEPS:
                        sol[x] = sol[x] - weight(64 + spot) * field
        for x in range(2):
            solution_ref[b, :, x] = sol[x]
            residual_ref[b, :, x] = res[x]


def solution(mesh):
    n_gx, n_gy = mesh.shape["gx"], mesh.shape["gy"]
    n_z = 8 if n_gx % 8 == 0 else n_gx
    n_y = n_gx // n_z
    cosine, sine = phase_tables()

    def shards(right_side, stencil, class_scale, material, boundary, sign_bits, sample_rows):
        rhs = jnp.transpose(right_side, (0, 1, 3, 2, 4))
        signs = jnp.transpose(sign_bits, (0, 2, 1, 3))
        blocks = jnp.transpose(stencil, (1, 2, 0))
        vmem = pl.BlockSpec(memory_space=pltpu.VMEM)
        smem = pl.BlockSpec(memory_space=pltpu.SMEM)
        hbm = pl.BlockSpec(memory_space=pl.ANY)
        out = pltpu.VMEM((BW, 3, 2, 16, 128), jnp.float32)
        most = max(n_gy, n_y, n_z)
        answer, residual = pl.pallas_call(
            lambda *refs: cycle_kernel(n_gx, n_gy, n_y, n_z, *refs),
            out_shape=(out, out),
            in_specs=[smem, hbm] + [vmem] * 7,
            out_specs=(vmem, vmem),
            scratch_shapes=[
                pltpu.VMEM((NV, BW, 3, 6, 32, 128), jnp.float32),
                pltpu.VMEM((4, 32, 128), jnp.float32),
                pltpu.VMEM((4, 32, 128), jnp.float32),
                pltpu.VMEM((4, 32, 128), jnp.float32),
                pltpu.VMEM((96, 128), jnp.float32),
                pltpu.VMEM((128, 128), jnp.bfloat16),
                pltpu.VMEM((16, 128), jnp.float32),
                pltpu.SMEM((16, 128), jnp.float32),
                pltpu.VMEM((128, 128), jnp.float32),
                pltpu.VMEM((GROUPS, n_gy, 2 * BW, 128), jnp.float32),
                pltpu.VMEM((GROUPS, n_y, 2 * BW, 128), jnp.float32),
                pltpu.VMEM((GROUPS, n_z, 2 * BW, 128), jnp.float32),
                pltpu.SemaphoreType.DMA((PAIRS, BW, 8)),
                pltpu.SemaphoreType.DMA((PAIRS, BW, 8)),
                pltpu.SemaphoreType.DMA((8,)),
                pltpu.SemaphoreType.DMA((8,)),
                pltpu.SemaphoreType.DMA((3 * BW,)),
                pltpu.SemaphoreType.DMA((3, GROUPS, most)),
                pltpu.SemaphoreType.DMA((3, GROUPS, most)),
                pltpu.SemaphoreType.DMA,
            ],
            compiler_params=pltpu.CompilerParams(collective_id=0, has_side_effects=True),
            name="cycle",
        )(
            class_scale, rhs, blocks, material, boundary, signs, sample_rows.reshape(1, 128),
            cosine, sine,
        )
        back = lambda t: jnp.transpose(t, (2, 3, 0, 1, 4))
        return back(answer), back(residual)

    return jax.shard_map(
        shards,
        mesh=mesh,
        in_specs=(
            P("gx", "gy", None, None, None),
            P(),
            P(),
            P("gx", "gy", None),
            P("gx", "gy", None),
            P("gx", "gy", None, None),
            P("gx", "gy", None),
        ),
        out_specs=(P("gx", "gy", None, None, None), P("gx", "gy", None, None, None)),
        check_vma=False,
    )
```
